32 devices in a mesh: rep: 1 (over z), r: 4 (over y), s: 8 (over x, core).
Axes of the slice: x: 4, y: 4, z: 1, core: 2. Of those that a mesh axis runs over, the one named last changes fastest.
The devices are a block of a 4x4x8 slice.
Arguments:
- x: bfloat16 [32, 2048, 896], P(('rep', 'r', 's'))
- dy: bfloat16 [32, 2048, 896], P(('rep', 'r', 's'))
- w_gate: bfloat16 [2, 896, 3584], P(None, 's')
- w_up: bfloat16 [2, 896, 3584], P(None, 's')
- w_down: bfloat16 [2, 3584, 896], P(None, 's')
Outputs:
- output 1: bfloat16 [32, 2048, 896], P(('rep', 'r', 's'))
- output 2: bfloat16 [2, 896, 3584], P('rep', 's')
- output 3: bfloat16 [2, 896, 3584], P('rep', 's')
- output 4: bfloat16 [2, 3584, 896], P('rep', 's')
All inputs are finite; a program needn't handle non-finite values.
Results may differ from the reference program's by a relative error of at most 0.018.
Values are sent between devices in bfloat16 or wider.
A program may use at most 768 MiB of HBM per device.

```python
import jax
import jax.numpy as jnp
from jax import lax

SEQUENCES = 32
TOKENS = 2048
D = 896
FF = 3584
LAYERS = 2
NAMES = ("w_gate", "w_up", "w_down")
SHAPES = {"w_gate": (LAYERS, D, FF), "w_up": (LAYERS, D, FF), "w_down": (LAYERS, FF, D)}


def bump(key, n, height):
    away = (jnp.arange(n, dtype=jnp.int32) - jax.random.randint(key, (), 0, n, jnp.int32)) % n
    return jnp.where(away < n // 8, height, 1.0)


def together(key, own, strength):
    shared = jax.random.normal(key, own.shape[1:], jnp.float32)
    return (own + strength * shared) * lax.rsqrt(1 + strength * strength)


def setup_inputs(seed: int = 0, part: int = 0) -> dict:
    kx, kdy, ka, kb, kz, kf, kh, kl, *kw = jax.random.split(jax.random.key(seed), 8 + len(NAMES))
    kx, kdy, ka, kb = (jax.random.fold_in(k, part) for k in (kx, kdy, ka, kb))
    shape = (SEQUENCES, TOKENS, D)
    much_x, much_dy = jax.random.uniform(kz, (2,), jnp.float32, 0.0, 1.0)
    layers = 2.0 ** jax.random.uniform(kl, (LAYERS, 1, 1), jnp.float32, -1.0, 1.0)
    x = together(ka, jax.random.normal(kx, shape, jnp.float32), much_x) * bump(kf, D, 4.0)
    dy = together(kb, jax.random.normal(kdy, shape, jnp.float32), much_dy)
    drawn = {"x": x.astype(jnp.bfloat16), "dy": (dy * (SEQUENCES * TOKENS) ** -0.5).astype(jnp.bfloat16)}
    for key, name in zip(kw, NAMES, strict=True):
        w = jax.random.normal(key, SHAPES[name], jnp.float32) * SHAPES[name][1] ** -0.5
        drawn[name] = (w * {"w_gate": 1.0, "w_up": bump(kh, FF, 4.0), "w_down": layers}[name]).astype(jnp.bfloat16)
    return drawn


def matmul(a, w):
    return jnp.dot(a, w, preferred_element_type=jnp.float32).astype(jnp.bfloat16)


def normed(h):
    wide = h.astype(jnp.float32)
    scale = lax.rsqrt(jnp.mean(wide**2, -1, keepdims=True) + 1e-6)
    return (wide * scale).astype(jnp.bfloat16)


def layer(h, w):
    a = normed(h)
    gate = jnp.dot(a, w["w_gate"], preferred_element_type=jnp.float32)
    up = jnp.dot(a, w["w_up"], preferred_element_type=jnp.float32)
    return h + matmul((jax.nn.silu(gate) * up).astype(jnp.bfloat16), w["w_down"])


def stack(weights, h):
    return lax.scan(lambda h, w: (layer(h, w), None), h, weights)[0]


def reference(x, dy, w_gate, w_up, w_down):
    weights = dict(zip(NAMES, (w_gate, w_up, w_down), strict=True))

    def take(so_far, sequence):
        h, by_y = sequence
        _, back = jax.vjp(stack, weights, h)
        by_weights, by_h = back(by_y)
        return jax.tree.map(lambda total, term: total + term.astype(jnp.float32), so_far, by_weights), by_h

    none_yet = {name: jnp.zeros(w.shape, jnp.float32) for name, w in weights.items()}
    by_weights, by_x = lax.scan(take, none_yet, (x, dy))
    return (by_x, *(by_weights[name].astype(jnp.bfloat16) for name in NAMES))
```

```python
import functools

import jax
import jax.numpy as jnp
from jax import lax
from jax.experimental import pallas as pl
from jax.experimental.pallas import tpu as pltpu
from jax.sharding import PartitionSpec as P

F32 = jnp.float32
BF16 = jnp.bfloat16
ANY = pl.BlockSpec(memory_space=pl.ANY)
MESH = pl.DeviceIdType.MESH
BLOCK = 512
LANES = 128
VMEM_LIMIT = 67_000_000


def dot(a, b):
    return lax.dot_general(a, b, (((1,), (0,)), ((), ())), preferred_element_type=F32)


def dot_t(a, b):
    return lax.dot_general(a, b, (((1,), (1,)), ((), ())), preferred_element_type=F32)


def rows_of(start, size):
    return pl.ds(pl.multiple_of(start, 16), size)


def lanes_of(start, size):
    return pl.ds(pl.multiple_of(start, LANES), size)


def wait_for(ref, sem):
    pltpu.make_async_copy(ref, ref, sem).wait()


class Place:
    def __init__(self, nr, ns):
        self.nr, self.nx = nr, ns // 2
        self.r, self.s = lax.axis_index("r"), lax.axis_index("s")
        self.x, self.c = self.s // 2, self.s % 2

    def at(self, dx=0, dy=0, dc=0):
        return {"r": (self.r + dy) % self.nr, "s": 2 * ((self.x + dx) % self.nx) + (self.c + dc) % 2}

    def row(self, dx):
        return 2 * ((self.x + dx) % self.nx) + self.c


def send(src, dst, send_sem, recv_sem, device):
    pltpu.make_async_remote_copy(src_ref=src, dst_ref=dst, send_sem=send_sem, recv_sem=recv_sem, device_id=device, device_id_type=MESH).start()


def greet(peers):
    barrier = pltpu.get_barrier_semaphore()
    for peer in peers:
        pl.semaphore_signal(barrier, inc=1, device_id=peer, device_id_type=MESH)
    pl.semaphore_wait(barrier, len(peers))


class Gather:
    def __init__(self, place, nb, shard_rows, down_rows, own, whole, sems):
        self.p, self.nb, self.m, self.dr = place, nb, shard_rows, down_rows
        self.own, self.whole = own, whole
        self.x1s, self.x1r, self.x2s, self.x2r, self.ys, self.yr, self.ds, self.dr_, self.loc = sems
        self.half = place.r % 2
        self.quarter_rows = down_rows // nb // 4

    def piece(self, i):
        n = i % self.nb
        return i // self.nb, 4 * (n % 2) + n // 2, n

    def src(self, i, q, n=1):
        layer, j, t = self.piece(i)
        width = self.nb * LANES
        for k in range(2):
            for e in range(n):
                yield self.own[k].at[layer, :, lanes_of(width * (q + e) + LANES * j, LANES)]
        yield self.own[2].at[layer, rows_of(4 * self.quarter_rows * t + self.quarter_rows * q, n * self.quarter_rows), :]

    def dst(self, i, s, q, n=1, split=False):
        layer, j, t = self.piece(i)
        for k in range(2):
            if split:
                for e in range(n):
                    yield self.whole[k].at[layer, j, rows_of(self.m * s, self.m), lanes_of(LANES * (q + e), LANES)]
            else:
                yield self.whole[k].at[layer, j, rows_of(self.m * s, self.m), lanes_of(LANES * q, n * LANES)]
        yield self.whole[2].at[layer, rows_of(self.dr * s + 4 * self.quarter_rows * t + self.quarter_rows * q, n * self.quarter_rows), :]

    def units(self, a, b, c=1):
        if c == 1:
            return self.whole[0].at[0, 0, : self.m * a, : LANES * b]
        return self.whole[0].at[0, :c, : self.m * a, : LANES * b]

    def first(self, i):
        s = self.p.s
        for d, dx in enumerate((1, -1)):
            for a, b in zip(self.src(i, 2 * self.half, 2), self.dst(i, s, 2 * self.half, 2, True)):
                send(a, b, self.x1s.at[i], self.x1r.at[i, d], self.p.at(dx=dx))
        for a, b in zip(self.src(i, 0, 4), self.dst(i, s, 0, 4, True)):
            send(a, b, self.x1s.at[i], self.dr_.at[i], self.p.at(dc=1))
            pltpu.make_async_copy(a, b, self.loc.at[i]).start()

    def second(self, i):
        for d, dx in enumerate((1, -1)):
            wait_for(self.units(6, 1), self.x1r.at[i, d])
            for a in self.dst(i, self.p.row(-dx), 2 * self.half + d):
                send(a, a, self.x2s.at[i], self.x2r.at[i, d], self.p.at(dx=dx))

    def third(self, i):
        for d in range(2):
            wait_for(self.units(3, 1), self.x2r.at[i, d])
        for d, dy in enumerate((1, -1)):
            for dx in (1, -1, 2):
                for a in self.dst(i, self.p.row(dx), 2 * self.half + d):
                    send(a, a, self.ys.at[i], self.yr.at[i, d], self.p.at(dy=dy))

    def fourth(self, i):
        for d in range(2):
            wait_for(self.units(3, 3), self.yr.at[i, d])
        for dx in (1, -1, 2):
            for a in self.dst(i, self.p.row(dx), 0, 4):
                send(a, a, self.ds.at[i], self.dr_.at[i], self.p.at(dc=1))

    def ready(self, i):
        wait_for(self.units(6, 4, 2), self.dr_.at[i])
        wait_for(self.units(3, 4), self.loc.at[i])

    def sent(self, i):
        wait_for(self.units(6, 4), self.x1s.at[i])
        wait_for(self.units(6, 1), self.x2s.at[i])
        wait_for(self.units(6, 3), self.ys.at[i])
        wait_for(self.units(6, 3, 2), self.ds.at[i])


def normed(h):
    return h * lax.rsqrt(jnp.mean(h * h, -1, keepdims=True) + 1e-6)


def silu(g):
    return g * (jnp.tanh(g * 0.5) * 0.5 + 0.5)


def forward_kernel(nr, ns, x_h, dy_h, og_h, ou_h, od_h, a0_h, xt_h, dyt_h, a1_h, h1t_h, wg_h, wu_h, wd_h, x, a, t1, acc, act, og, ou, od, wg, wu, wd, x1s, x1r, x2s, x2r, ys, yr, ds, dr, loc, io, wsem):
    place = Place(nr, ns)
    tokens, d = x.shape
    nb = wg_h.shape[1]
    pieces = wg_h.shape[0] * nb
    loads = [pltpu.make_async_copy(p, q, io.at[k]) for k, (p, q) in enumerate(((og_h, og), (ou_h, ou), (od_h, od), (x_h, x)))]
    for load in loads:
        load.start()
    greet([place.at(dx=1), place.at(dx=-1), place.at(dy=1), place.at(dy=-1), place.at(dc=1)])
    gather = Gather(place, nb, og.shape[1], od.shape[1], (og, ou, od), (wg_h, wu_h, wd_h), (x1s, x1r, x2s, x2r, ys, yr, ds, dr, loc))
    for load in loads[:3]:
        load.wait()
    gather.first(0)
    loads[3].wait()
    small = 256

    def prepare(k, carry):
        rows = pl.ds(pl.multiple_of(k * small, small), small)
        a[rows, :] = normed(x[rows, :].astype(F32)).astype(BF16)
        t1[:, rows] = x[rows, :].T
        return carry

    lax.fori_loop(0, tokens // small, prepare, 0)
    outs = [pltpu.make_async_copy(a, a0_h, io.at[0]), pltpu.make_async_copy(t1, xt_h, io.at[1])]
    for out in outs:
        out.start()
    acc[...] = jnp.zeros_like(acc)

    def load_up(i, slot):
        _, j, _ = gather.piece(i)
        return [pltpu.make_async_copy(h.at[0, j], v.at[slot], wsem.at[slot, k]) for k, (h, v) in enumerate(((wg_h, wg), (wu_h, wu)))]

    def load_down(i):
        _, j, _ = gather.piece(i)
        return [pltpu.make_async_copy(wd_h.at[0, rows_of(q * nb * LANES + LANES * j, LANES), :], wd.at[pl.ds(q * LANES, LANES), :], wsem.at[2, q]) for q in range(4)]

    big = 1024

    def step(k, carry):
        def stage(run, lag):
            @pl.when((k >= lag) & (k - lag < pieces))
            def _():
                run(k - lag)

        @pl.when((k >= 1) & (k < pieces))
        def _():
            gather.first(k)

        stage(gather.second, 1)
        stage(gather.third, 2)
        stage(gather.fourth, 3)
        stage(gather.ready, 4)

        @pl.when((k >= 4) & (k < 4 + nb))
        def _():
            for load in load_up(k - 4, k % 2):
                load.start()

        @pl.when((k >= 5) & (k < 5 + nb))
        def _():
            i = k - 5
            slot = (k - 1) % 2
            for load in load_down(i):
                load.start()
            for load in load_up(i, slot):
                load.wait()

            def up(n, carry):
                rows = pl.ds(pl.multiple_of(n * big, big), big)
                g = dot(a[rows, :], wg[slot])
                u = dot(a[rows, :], wu[slot])
                act[rows, :] = (silu(g) * u).astype(BF16)
                return carry

            lax.fori_loop(0, tokens // big, up, 0)
            for load in load_down(i):
                load.wait()

            def down(n, carry):
                rows = pl.ds(pl.multiple_of(n * big, big), big)
                acc[rows, :] += dot(act[rows, :], wd[...])
                return carry

            lax.fori_loop(0, tokens // big, down, 0)

        return carry

    lax.fori_loop(0, pieces + 5, step, 0)
    for out in outs:
        out.wait()

    def finish(k, carry):
        rows = pl.ds(pl.multiple_of(k * small, small), small)
        h = (x[rows, :].astype(F32) + acc[rows, :].astype(BF16).astype(F32)).astype(BF16)
        a[rows, :] = normed(h.astype(F32)).astype(BF16)
        t1[:, rows] = h.T
        return carry

    lax.fori_loop(0, tokens // small, finish, 0)
    outs = [pltpu.make_async_copy(a, a1_h, io.at[0]), pltpu.make_async_copy(t1, h1t_h, io.at[1])]
    for out in outs:
        out.start()
    load = pltpu.make_async_copy(dy_h, x, io.at[2])
    load.start()
    for out in outs:
        out.wait()
    load.wait()

    def turn(k, carry):
        rows = pl.ds(pl.multiple_of(k * small, small), small)
        t1[:, rows] = x[rows, :].T
        return carry

    lax.fori_loop(0, tokens // small, turn, 0)
    out = pltpu.make_async_copy(t1, dyt_h, io.at[0])
    out.start()
    out.wait()

    def drain(i, carry):
        gather.sent(i)
        return carry

    lax.fori_loop(0, pieces, drain, 0)


def forward(mesh, x, dy, w_gate, w_up, w_down):
    nr, ns = mesh.shape["r"], mesh.shape["s"]
    tokens, d = x.shape
    layers, m, hidden = w_gate.shape
    nb = hidden // BLOCK
    pieces = layers * nb
    states, turned = jax.ShapeDtypeStruct((tokens, d), BF16), jax.ShapeDtypeStruct((d, tokens), BF16)
    up = jax.ShapeDtypeStruct((layers, nb, d, BLOCK), BF16)
    dma = pltpu.SemaphoreType.DMA
    return pl.pallas_call(
        functools.partial(forward_kernel, nr, ns),
        out_shape=(states, turned, turned, states, turned, up, up, jax.ShapeDtypeStruct((layers, hidden, d), BF16)),
        in_specs=[ANY] * 5,
        out_specs=(ANY,) * 8,
        scratch_shapes=[
            pltpu.VMEM((tokens, d), BF16),
            pltpu.VMEM((tokens, d), BF16),
            pltpu.VMEM((d, tokens), BF16),
            pltpu.VMEM((tokens, d), F32),
            pltpu.VMEM((tokens, BLOCK), BF16),
            pltpu.VMEM(w_gate.shape, BF16),
            pltpu.VMEM(w_up.shape, BF16),
            pltpu.VMEM(w_down.shape, BF16),
            pltpu.VMEM((2, d, BLOCK), BF16),
            pltpu.VMEM((2, d, BLOCK), BF16),
            pltpu.VMEM((BLOCK, d), BF16),
            dma((pieces,)),
            dma((pieces, 2)),
            dma((pieces,)),
            dma((pieces, 2)),
            dma((pieces,)),
            dma((pieces, 2)),
            dma((pieces,)),
            dma((pieces,)),
            dma((pieces,)),
            dma((4,)),
            dma((3, 4)),
        ],
        compiler_params=pltpu.CompilerParams(collective_id=0, has_side_effects=True, vmem_limit_bytes=VMEM_LIMIT),
        name="forward",
    )(x, dy, w_gate, w_up, w_down)


NAMES = ("w_gate", "w_up", "w_down")


def matmul(a, w):
    return jnp.dot(a, w, preferred_element_type=jnp.float32).astype(jnp.bfloat16)


def normed0(h):
    wide = h.astype(jnp.float32)
    scale = lax.rsqrt(jnp.mean(wide**2, -1, keepdims=True) + 1e-6)
    return (wide * scale).astype(jnp.bfloat16)


def layer(h, w):
    a = normed0(h)
    gate = jnp.dot(a, w["w_gate"], preferred_element_type=jnp.float32)
    up = jnp.dot(a, w["w_up"], preferred_element_type=jnp.float32)
    return h + matmul((jax.nn.silu(gate) * up).astype(jnp.bfloat16), w["w_down"])


def solution(mesh):
    def summed(term):
        return lax.psum(lax.psum_scatter(term, "s", scatter_dimension=0, tiled=True), "r")

    def step(x, dy, *weights):
        layers, _, hidden = weights[0].shape
        d = x.shape[-1]
        nb = hidden // BLOCK
        a0, xt, dyt, a1, h1t, wg, wu, wd = forward(mesh, x[0], dy[0], *weights)

        def whole(w):
            return w.reshape(layers, nb, d, 4, LANES).transpose(0, 2, 3, 1, 4).reshape(layers, d, hidden)

        full = (whole(wg), whole(wu), wd)
        inputs = [xt.T, h1t.T]
        by_h, mine = dyt.T, [None] * layers
        for number in reversed(range(layers)):
            w = {name: full[k][number] for k, name in enumerate(NAMES)}
            _, back = jax.vjp(lambda w, h: layer(h, w), w, inputs[number])
            by_w, by_h = back(by_h)
            mine[number] = [summed(by_w[name]) for name in NAMES]
        return (by_h[None], *(jnp.stack([mine[number][i] for number in range(layers)]) for i in range(3)))

    states, cut = P(("rep", "r", "s"), None, None), P(None, "s", None)
    return jax.shard_map(
        step,
        mesh=mesh,
        in_specs=(states, states) + (cut,) * 3,
        out_specs=(states,) + (P("rep", "s", None),) * 3,
        check_vma=False,
    )
```

```python
import functools

import jax
import jax.numpy as jnp
from jax import lax
from jax.experimental import pallas as pl
from jax.experimental.pallas import tpu as pltpu
from jax.sharding import PartitionSpec as P

F32 = jnp.float32
BF16 = jnp.bfloat16
ANY = pl.BlockSpec(memory_space=pl.ANY)
MESH = pl.DeviceIdType.MESH
BLOCK = 512
LANES = 128
VMEM_LIMIT = 67_000_000


def dot(a, b):
    return lax.dot_general(a, b, (((1,), (0,)), ((), ())), preferred_element_type=F32)


def dot_t(a, b):
    return lax.dot_general(a, b, (((1,), (1,)), ((), ())), preferred_element_type=F32)


def rows_of(start, size):
    return pl.ds(pl.multiple_of(start, 16), size)


def lanes_of(start, size):
    return pl.ds(pl.multiple_of(start, LANES), size)


def wait_for(ref, sem):
    pltpu.make_async_copy(ref, ref, sem).wait()


class Place:
    def __init__(self, nr, ns):
        self.nr, self.nx = nr, ns // 2
        self.r, self.s = lax.axis_index("r"), lax.axis_index("s")
        self.x, self.c = self.s // 2, self.s % 2

    def at(self, dx=0, dy=0, dc=0):
        return {"r": (self.r + dy) % self.nr, "s": 2 * ((self.x + dx) % self.nx) + (self.c + dc) % 2}

    def row(self, dx):
        return 2 * ((self.x + dx) % self.nx) + self.c


def send(src, dst, send_sem, recv_sem, device):
    pltpu.make_async_remote_copy(src_ref=src, dst_ref=dst, send_sem=send_sem, recv_sem=recv_sem, device_id=device, device_id_type=MESH).start()


def greet(peers):
    barrier = pltpu.get_barrier_semaphore()
    for peer in peers:
        pl.semaphore_signal(barrier, inc=1, device_id=peer, device_id_type=MESH)
    pl.semaphore_wait(barrier, len(peers))


class Gather:
    def __init__(self, place, nb, shard_rows, down_rows, own, whole, sems):
        self.p, self.nb, self.m, self.dr = place, nb, shard_rows, down_rows
        self.own, self.whole = own, whole
        self.x1s, self.x1r, self.x2s, self.x2r, self.ys, self.yr, self.ds, self.dr_, self.loc = sems
        self.half = place.r % 2
        self.quarter_rows = down_rows // nb // 4

    def piece(self, i):
        n = i % self.nb
        return i // self.nb, 4 * (n % 2) + n // 2, n

    def src(self, i, q, n=1):
        layer, j, t = self.piece(i)
        width = self.nb * LANES
        for k in range(2):
            for e in range(n):
                yield self.own[k].at[layer, :, lanes_of(width * (q + e) + LANES * j, LANES)]
        yield self.own[2].at[layer, rows_of(4 * self.quarter_rows * t + self.quarter_rows * q, n * self.quarter_rows), :]

    def dst(self, i, s, q, n=1, split=False):
        layer, j, t = self.piece(i)
        for k in range(2):
            if split:
                for e in range(n):
                    yield self.whole[k].at[layer, j, rows_of(self.m * s, self.m), lanes_of(LANES * (q + e), LANES)]
            else:
                yield self.whole[k].at[layer, j, rows_of(self.m * s, self.m), lanes_of(LANES * q, n * LANES)]
        yield self.whole[2].at[layer, rows_of(self.dr * s + 4 * self.quarter_rows * t + self.quarter_rows * q, n * self.quarter_rows), :]

    def units(self, a, b, c=1):
        if c == 1:
            return self.whole[0].at[0, 0, : self.m * a, : LANES * b]
        return self.whole[0].at[0, :c, : self.m * a, : LANES * b]

    def first(self, i):
        s = self.p.s
        for d, dx in enumerate((1, -1)):
            for a, b in zip(self.src(i, 2 * self.half, 2), self.dst(i, s, 2 * self.half, 2, True)):
                send(a, b, self.x1s.at[i], self.x1r.at[i, d], self.p.at(dx=dx))
        for a, b in zip(self.src(i, 0, 4), self.dst(i, s, 0, 4, True)):
            send(a, b, self.x1s.at[i], self.dr_.at[i], self.p.at(dc=1))
            pltpu.make_async_copy(a, b, self.loc.at[i]).start()

    def second(self, i):
        for d, dx in enumerate((1, -1)):
            wait_for(self.units(6, 1), self.x1r.at[i, d])
            for a in self.dst(i, self.p.row(-dx), 2 * self.half + d):
                send(a, a, self.x2s.at[i], self.x2r.at[i, d], self.p.at(dx=dx))

    def third(self, i):
        for d in range(2):
            wait_for(self.units(3, 1), self.x2r.at[i, d])
        for d, dy in enumerate((1, -1)):
            for dx in (1, -1, 2):
                for a in self.dst(i, self.p.row(dx), 2 * self.half + d):
                    send(a, a, self.ys.at[i], self.yr.at[i, d], self.p.at(dy=dy))

    def fourth(self, i):
        for d in range(2):
            wait_for(self.units(3, 3), self.yr.at[i, d])
        for dx in (1, -1, 2):
            for a in self.dst(i, self.p.row(dx), 0, 4):
                send(a, a, self.ds.at[i], self.dr_.at[i], self.p.at(dc=1))

    def ready(self, i):
        wait_for(self.units(6, 4, 2), self.dr_.at[i])
        wait_for(self.units(3, 4), self.loc.at[i])

    def sent(self, i):
        wait_for(self.units(6, 4), self.x1s.at[i])
        wait_for(self.units(6, 1), self.x2s.at[i])
        wait_for(self.units(6, 3), self.ys.at[i])
        wait_for(self.units(6, 3, 2), self.ds.at[i])


def normed(h):
    return h * lax.rsqrt(jnp.mean(h * h, -1, keepdims=True) + 1e-6)


def silu(g):
    return g * (jnp.tanh(g * 0.5) * 0.5 + 0.5)


def forward_kernel(nr, ns, x_h, dy_h, og_h, ou_h, od_h, a0_h, xt_h, dyt_h, a1_h, h1t_h, wg_h, wu_h, wd_h, x, a, t1, acc, act, og, ou, od, wg, wu, wd, x1s, x1r, x2s, x2r, ys, yr, ds, dr, loc, io, wsem):
    place = Place(nr, ns)
    tokens, d = x.shape
    nb = wg_h.shape[1]
    pieces = wg_h.shape[0] * nb
    loads = [pltpu.make_async_copy(p, q, io.at[k]) for k, (p, q) in enumerate(((og_h, og), (ou_h, ou), (od_h, od), (x_h, x)))]
    for load in loads:
        load.start()
    greet([place.at(dx=1), place.at(dx=-1), place.at(dy=1), place.at(dy=-1), place.at(dc=1)])
    gather = Gather(place, nb, og.shape[1], od.shape[1], (og, ou, od), (wg_h, wu_h, wd_h), (x1s, x1r, x2s, x2r, ys, yr, ds, dr, loc))
    for load in loads[:3]:
        load.wait()
    gather.first(0)
    loads[3].wait()
    small = 256

    def prepare(k, carry):
        rows = pl.ds(pl.multiple_of(k * small, small), small)
        a[rows, :] = normed(x[rows, :].astype(F32)).astype(BF16)
        t1[:, rows] = x[rows, :].T
        return carry

    lax.fori_loop(0, tokens // small, prepare, 0)
    outs = [pltpu.make_async_copy(a, a0_h, io.at[0]), pltpu.make_async_copy(t1, xt_h, io.at[1])]
    for out in outs:
        out.start()
    acc[...] = jnp.zeros_like(acc)

    def load_up(i, slot):
        _, j, _ = gather.piece(i)
        return [pltpu.make_async_copy(h.at[0, j], v.at[slot], wsem.at[slot, k]) for k, (h, v) in enumerate(((wg_h, wg), (wu_h, wu)))]

    def load_down(i):
        _, j, _ = gather.piece(i)
        return [pltpu.make_async_copy(wd_h.at[0, rows_of(q * nb * LANES + LANES * j, LANES), :], wd.at[pl.ds(q * LANES, LANES), :], wsem.at[2, q]) for q in range(4)]

    big = 1024

    def step(k, carry):
        def stage(run, lag):
            @pl.when((k >= lag) & (k - lag < pieces))
            def _():
                run(k - lag)

        @pl.when((k >= 1) & (k < pieces))
        def _():
            gather.first(k)

        stage(gather.second, 1)
        stage(gather.third, 2)
        stage(gather.fourth, 3)
        stage(gather.ready, 4)

        @pl.when((k >= 4) & (k < 4 + nb))
        def _():
            for load in load_up(k - 4, k % 2):
                load.start()

        @pl.when((k >= 5) & (k < 5 + nb))
        def _():
            i = k - 5
            slot = (k - 1) % 2
            for load in load_down(i):
                load.start()
            for load in load_up(i, slot):
                load.wait()

            def up(n, carry):
                rows = pl.ds(pl.multiple_of(n * big, big), big)
                g = dot(a[rows, :], wg[slot])
                u = dot(a[rows, :], wu[slot])
                act[rows, :] = (silu(g) * u).astype(BF16)
                return carry

            lax.fori_loop(0, tokens // big, up, 0)
            for load in load_down(i):
                load.wait()

            def down(n, carry):
                rows = pl.ds(pl.multiple_of(n * big, big), big)
                acc[rows, :] += dot(act[rows, :], wd[...])
                return carry

            lax.fori_loop(0, tokens // big, down, 0)

        return carry

    lax.fori_loop(0, pieces + 5, step, 0)
    for out in outs:
        out.wait()

    def finish(k, carry):
        rows = pl.ds(pl.multiple_of(k * small, small), small)
        h = (x[rows, :].astype(F32) + acc[rows, :].astype(BF16).astype(F32)).astype(BF16)
        a[rows, :] = normed(h.astype(F32)).astype(BF16)
        t1[:, rows] = h.T
        return carry

    lax.fori_loop(0, tokens // small, finish, 0)
    outs = [pltpu.make_async_copy(a, a1_h, io.at[0]), pltpu.make_async_copy(t1, h1t_h, io.at[1])]
    for out in outs:
        out.start()
    load = pltpu.make_async_copy(dy_h, x, io.at[2])
    load.start()
    for out in outs:
        out.wait()
    load.wait()

    def turn(k, carry):
        rows = pl.ds(pl.multiple_of(k * small, small), small)
        t1[:, rows] = x[rows, :].T
        return carry

    lax.fori_loop(0, tokens // small, turn, 0)
    out = pltpu.make_async_copy(t1, dyt_h, io.at[0])
    out.start()
    out.wait()

    def drain(i, carry):
        gather.sent(i)
        return carry

    lax.fori_loop(0, pieces, drain, 0)


def forward(mesh, x, dy, w_gate, w_up, w_down):
    nr, ns = mesh.shape["r"], mesh.shape["s"]
    tokens, d = x.shape
    layers, m, hidden = w_gate.shape
    nb = hidden // BLOCK
    pieces = layers * nb
    states, turned = jax.ShapeDtypeStruct((tokens, d), BF16), jax.ShapeDtypeStruct((d, tokens), BF16)
    up = jax.ShapeDtypeStruct((layers, nb, d, BLOCK), BF16)
    dma = pltpu.SemaphoreType.DMA
    return pl.pallas_call(
        functools.partial(forward_kernel, nr, ns),
        out_shape=(states, turned, turned, states, turned, up, up, jax.ShapeDtypeStruct((layers, hidden, d), BF16)),
        in_specs=[ANY] * 5,
        out_specs=(ANY,) * 8,
        scratch_shapes=[
            pltpu.VMEM((tokens, d), BF16),
            pltpu.VMEM((tokens, d), BF16),
            pltpu.VMEM((d, tokens), BF16),
            pltpu.VMEM((tokens, d), F32),
            pltpu.VMEM((tokens, BLOCK), BF16),
            pltpu.VMEM(w_gate.shape, BF16),
            pltpu.VMEM(w_up.shape, BF16),
            pltpu.VMEM(w_down.shape, BF16),
            pltpu.VMEM((2, d, BLOCK), BF16),
            pltpu.VMEM((2, d, BLOCK), BF16),
            pltpu.VMEM((BLOCK, d), BF16),
            dma((pieces,)),
            dma((pieces, 2)),
            dma((pieces,)),
            dma((pieces, 2)),
            dma((pieces,)),
            dma((pieces, 2)),
            dma((pieces,)),
            dma((pieces,)),
            dma((pieces,)),
            dma((4,)),
            dma((3, 4)),
        ],
        compiler_params=pltpu.CompilerParams(collective_id=0, has_side_effects=True, vmem_limit_bytes=VMEM_LIMIT),
        name="forward",
    )(x, dy, w_gate, w_up, w_down)


class Reduce:
    def __init__(self, place, nb, layers, terms, pair, hop1, hop2, side, final, outs, sems):
        self.p, self.nb, self.layers = place, nb, layers
        self.tg, self.td = terms
        self.pg, self.pd = pair
        self.h1g, self.h1d = hop1
        self.h2g, self.h2d = hop2
        self.sg, self.sd = side
        self.fg, self.fd = final
        self.og, self.ou, self.od = outs
        self.ps, self.pr, self.h1s, self.h1r, self.h2s, self.h2r, self.ss, self.sr, self.fs, self.fl, self.fx, self.rg, self.rd = sems
        self.m = self.pg.shape[3]

    def own_rows(self, x, c):
        return rows_of(self.m * (2 * x + c), self.m)

    def down_rows(self, x, c):
        return rows_of(128 * x + 64 * c, 64)

    def at_x(self, dx):
        return (self.p.x + dx) % self.p.nx

    def units(self, a, b):
        return self.tg.at[0, 0, : self.m * a, : LANES * b]

    def pair_gate(self, b, k):
        slot, other = b % 3, 1 - self.p.c
        for x in range(self.p.nx):
            send(self.tg.at[slot, k, self.own_rows(x, other), :], self.pg.at[slot, x, k], self.ps.at[slot], self.pr.at[slot], self.p.at(dc=1))

    def pair_down(self, b):
        slot, other = b % 3, 1 - self.p.c
        for x in range(self.p.nx):
            send(self.td.at[slot, self.down_rows(x, other), :], self.pd.at[slot, x], self.ps.at[slot], self.pr.at[slot], self.p.at(dc=1))

    def both(self, slot, x, k, cols=None):
        cols = slice(None) if cols is None else cols
        return self.tg[slot, k, self.own_rows(x, self.p.c), cols].astype(F32) + self.pg[slot, x, k, :, cols].astype(F32)

    def both_down(self, slot, x, start=0, size=64):
        mine = self.td[slot, rows_of(128 * x + 64 * self.p.c + start, size), :].astype(F32)
        return mine + self.pd[slot, x, pl.ds(start, size), :].astype(F32)

    def first(self, b):
        slot, two = b % 3, b % 2
        wait_for(self.tg.at[0, :, : self.m * 6, :], self.ps.at[slot])
        wait_for(self.tg.at[0, :, : self.m * 6, :], self.pr.at[slot])
        x = self.at_x(2)
        for k in range(2):
            self.pg[slot, x, k] = self.both(slot, x, k).astype(BF16)
        self.pd[slot, x] = self.both_down(slot, x).astype(BF16)
        for d, dx in enumerate((1, -1)):
            for k in range(2):
                send(self.pg.at[slot, x, k, :, pl.ds(256 * d, 256)], self.h1g.at[two, d, k], self.h1s.at[two], self.h1r.at[two, d], self.p.at(dx=dx))
            send(self.pd.at[slot, x, pl.ds(32 * d, 32), :], self.h1d.at[two, d], self.h1s.at[two], self.h1r.at[two, d], self.p.at(dx=dx))

    def second(self, b):
        slot, two = b % 3, b % 2
        wait_for(self.units(6, 2), self.h1s.at[two])
        for d in range(2):
            wait_for(self.units(6, 1), self.h1r.at[two, d])
        for d, dx in enumerate((1, -1)):
            x = self.at_x(dx)
            with_hop, alone = slice(256 * d, 256 * d + 256), slice(256 - 256 * d, 512 - 256 * d)
            for k in range(2):
                self.pg[slot, x, k, :, with_hop] = (self.both(slot, x, k, with_hop) + self.h1g[two, d, k].astype(F32)).astype(BF16)
                self.pg[slot, x, k, :, alone] = self.both(slot, x, k, alone).astype(BF16)
            self.pd[slot, x, pl.ds(32 * d, 32), :] = (self.both_down(slot, x, 32 * d, 32) + self.h1d[two, d].astype(F32)).astype(BF16)
            self.pd[slot, x, pl.ds(32 - 32 * d, 32), :] = self.both_down(slot, x, 32 - 32 * d, 32).astype(BF16)
            for k in range(2):
                send(self.pg.at[slot, x, k], self.h2g.at[two, d, k], self.h2s.at[two], self.h2r.at[two, d], self.p.at(dx=dx))
            send(self.pd.at[slot, x], self.h2d.at[two, d], self.h2s.at[two], self.h2r.at[two, d], self.p.at(dx=dx))

    def chip_sum(self, b, k, q):
        slot, two = b % 3, b % 2
        cols = lanes_of(LANES * q, LANES)
        return self.both(slot, self.p.x, k, cols) + self.h2g[two, 0, k, :, cols].astype(F32) + self.h2g[two, 1, k, :, cols].astype(F32)

    def chip_sum_down(self, b, q):
        slot, two = b % 3, b % 2
        rows = rows_of(16 * q, 16)
        mine = self.td[slot, rows_of(128 * self.p.x + 64 * self.p.c + 16 * q, 16), :].astype(F32) + self.pd[slot, self.p.x, rows, :].astype(F32)
        return mine + self.h2d[two, 0, rows, :].astype(F32) + self.h2d[two, 1, rows, :].astype(F32)

    def third(self, b):
        slot, two = b % 3, b % 2
        wait_for(self.units(6, 4), self.h2s.at[two])
        for d in range(2):
            wait_for(self.units(3, 4), self.h2r.at[two, d])
        for dy in range(1, self.p.nr):
            q = (self.p.r + dy) % self.p.nr
            cols, rows = lanes_of(LANES * q, LANES), rows_of(16 * q, 16)
            for k in range(2):
                self.pg[slot, self.p.x, k, :, cols] = self.chip_sum(b, k, q).astype(BF16)
            self.pd[slot, self.p.x, rows, :] = self.chip_sum_down(b, q).astype(BF16)
            for k in range(2):
                send(self.pg.at[slot, self.p.x, k, :, cols], self.sg.at[two, dy - 1, k], self.ss.at[two], self.sr.at[two, dy - 1], self.p.at(dy=dy))
            send(self.pd.at[slot, self.p.x, rows, :], self.sd.at[two, dy - 1], self.ss.at[two], self.sr.at[two, dy - 1], self.p.at(dy=dy))

    def fourth(self, b):
        two = b % 2
        layer, j = self.layers - 1 - b // self.nb, b % self.nb
        wait_for(self.units(3, 3), self.ss.at[two])
        for n in range(self.p.nr - 1):
            wait_for(self.units(3, 1), self.sr.at[two, n])

        @pl.when(b >= 2)
        def _():
            self.final_sent(two)

        q = self.p.r
        for k in range(2):
            total = self.chip_sum(b, k, q)
            for n in range(self.p.nr - 1):
                total += self.sg[two, n, k].astype(F32)
            self.fg[two, k] = total.astype(BF16)
        total = self.chip_sum_down(b, q)
        for n in range(self.p.nr - 1):
            total += self.sd[two, n].astype(F32)
        self.fd[two] = total.astype(BF16)

        cols = lanes_of(self.nb * LANES * q + LANES * j, LANES)
        share = self.od.shape[1]
        place = 128 * j + 64 * self.p.c
        owner = place // share
        rows = rows_of(place + 16 * q - share * owner, 16)
        for dy in range(1, self.p.nr):
            for k, out in enumerate((self.og, self.ou)):
                send(self.fg.at[two, k], out.at[layer, :, cols], self.fs.at[two], self.rg.at[0], self.p.at(dy=dy))
            peer = {"r": (self.p.r + dy) % self.p.nr, "s": 2 * self.p.x + owner}
            send(self.fd.at[two], self.od.at[layer, rows, :], self.fs.at[two], self.rd.at[0], peer)
        for k, out in enumerate((self.og, self.ou)):
            pltpu.make_async_copy(self.fg.at[two, k], out.at[layer, :, cols], self.fl.at[two]).start()

        @pl.when(owner == self.p.c)
        def _():
            pltpu.make_async_copy(self.fd.at[two], self.od.at[layer, rows, :], self.fx.at[two]).start()

        @pl.when(owner != self.p.c)
        def _():
            send(self.fd.at[two], self.od.at[layer, rows, :], self.fx.at[two], self.rd.at[0], self.p.at(dc=1))

    def final_sent(self, two):
        wait_for(self.units(3, 3), self.fs.at[two])
        wait_for(self.units(2, 1), self.fl.at[two])
        wait_for(self.units(1, 1), self.fx.at[two])


def gates(g, u, d):
    sig = jnp.tanh(g * 0.5) * 0.5 + 0.5
    s = g * sig
    d = d.astype(BF16).astype(F32)
    return (s * u).astype(BF16), (d * u * (sig + s - s * sig)).astype(BF16), (d * s).astype(BF16)


def backward_kernel(
    nr, ns, dy_h, dyt_h, a0_h, xt_h, a1_h, h1t_h, wg_h, wu_h, wd_h, dx_h, gg_h, gu_h, gd_h,
    a, at, dy, dyt, ht, dat, act, dg, du, wg, wu, wd, tg, td, pg, pd, h1g, h1d, h2g, h2d, sg, sd, fg, fd,
    ps, pr, h1s, h1r, h2s, h2r, ss, sr, fs, fl, fx, rg, rd, io, wsem,
):
    place = Place(nr, ns)
    tokens, d = a.shape
    layers, nb = wg_h.shape[:2]
    steps = layers * nb
    loads = [pltpu.make_async_copy(p, q, io.at[k]) for k, (p, q) in enumerate(((h1t_h, at), (a1_h, a), (dy_h, dy), (dyt_h, dyt), (h1t_h, ht)))]
    for load in loads:
        load.start()

    def weights(b, slot):
        layer, j = layers - 1 - b // nb, b % nb
        yield pltpu.make_async_copy(wg_h.at[layer, j], wg.at[slot], wsem.at[slot, 0])
        yield pltpu.make_async_copy(wu_h.at[layer, j], wu.at[slot], wsem.at[slot, 1])
        for q in range(4):
            yield pltpu.make_async_copy(wd_h.at[layer, rows_of(q * nb * LANES + LANES * j, LANES), :], wd.at[slot, pl.ds(q * LANES, LANES), :], wsem.at[slot, 2 + q])

    for load in weights(0, 0):
        load.start()
    peers = [place.at(dx=1), place.at(dx=-1), place.at(dc=1)]
    for dy_ in range(1, nr):
        peers += [place.at(dy=dy_), place.at(dy=dy_, dc=1)]
    greet(peers)
    reduce = Reduce(
        place, nb, layers, (tg, td), (pg, pd), (h1g, h1d), (h2g, h2d), (sg, sd), (fg, fd), (gg_h, gu_h, gd_h),
        (ps, pr, h1s, h1r, h2s, h2r, ss, sr, fs, fl, fx, rg, rd),
    )
    small, big = 256, 1024

    def norm_turned():
        def chunk(n, carry):
            cols = pl.ds(pl.multiple_of(n * small, small), small)
            h = at[:, cols].astype(F32)
            at[:, cols] = (h * lax.rsqrt(jnp.mean(h * h, 0, keepdims=True) + 1e-6)).astype(BF16)
            return carry

        lax.fori_loop(0, tokens // small, chunk, 0)

    loads[0].wait()
    norm_turned()
    dat[...] = jnp.zeros_like(dat)
    for load in loads[1:]:
        load.wait()

    def layer_end(last):
        def chunk(n, carry):
            cols = pl.ds(pl.multiple_of(n * small, small), small)
            h = ht[:, cols].astype(F32)
            scale = lax.rsqrt(jnp.mean(h * h, 0, keepdims=True) + 1e-6)
            h = h * scale
            da = dat[:, cols].astype(BF16).astype(F32)
            v = dyt[:, cols].astype(F32) + scale * (da - h * jnp.mean(da * h, 0, keepdims=True))
            v = v.astype(BF16)
            if not last:
                dyt[:, cols] = v
                dat[:, cols] = jnp.zeros((d, small), F32)
            dy[cols, :] = v.T
            return carry

        lax.fori_loop(0, tokens // small, chunk, 0)

    def compute(k):
        slot = k % 2
        for load in weights(k, slot):
            load.wait()

        @pl.when(k + 1 < steps)
        def _():
            for load in weights(k + 1, 1 - slot):
                load.start()

        def chunk(n, carry):
            rows = pl.ds(pl.multiple_of(n * big, big), big)
            g = dot(a[rows, :], wg[slot])
            u = dot(a[rows, :], wu[slot])
            e = dot_t(dy[rows, :], wd[slot])
            act[rows, :], dg[rows, :], du[rows, :] = gates(g, u, e)
            return carry

        lax.fori_loop(0, tokens // big, chunk, 0)

    def terms(k):
        slot = k % 3
        for n, left in enumerate((dg, du)):
            for e in range(BLOCK // 256):
                cols = slice(256 * e, 256 * e + 256)
                tg[slot, n, :, cols] = dot(at[...], left[:, cols]).astype(BF16)
            reduce.pair_gate(k, n)
        for e in range(BLOCK // 256):
            cols = slice(256 * e, 256 * e + 256)
            td[slot, cols, :] = dot(dyt[...], act[:, cols]).astype(BF16).T
        reduce.pair_down(k)

    def back(k):
        slot = k % 2

        def chunk(n, carry):
            cols = pl.ds(pl.multiple_of(n * big, big), big)
            dat[:, cols] += dot_t(wg[slot], dg[cols, :]) + dot_t(wu[slot], du[cols, :])
            return carry

        lax.fori_loop(0, tokens // big, chunk, 0)

    def step(k, carry):
        def stage(run, lag):
            @pl.when((k >= lag) & (k - lag < steps))
            def _():
                run(k - lag)

        stage(reduce.third, 2)
        stage(reduce.first, 1)
        stage(compute, 0)

        @pl.when(k == steps)
        def _():
            pltpu.make_async_copy(xt_h, ht, io.at[4]).wait()
            layer_end(True)
            pltpu.make_async_copy(dy, dx_h, io.at[0]).start()

        stage(reduce.second, 1)
        stage(reduce.fourth, 2)
        stage(terms, 0)
        stage(back, 0)

        @pl.when(k == nb - 1)
        def _():
            loads = [pltpu.make_async_copy(p, q, io.at[n]) for n, (p, q) in enumerate(((a0_h, a), (xt_h, at)))]
            for load in loads:
                load.start()
            layer_end(False)
            pltpu.make_async_copy(xt_h, ht, io.at[4]).start()
            for load in loads:
                load.wait()
            norm_turned()

        return carry

    lax.fori_loop(0, steps + 2, step, 0)
    reduce.final_sent(0)
    reduce.final_sent(1)
    wait_for(wg_h.at[0, :3, : 7 * place_rows(gg_h), :], rg.at[0])
    wait_for(wg_h.at[0, :2, : 6 * place_rows(gg_h), :], rd.at[0])
    pltpu.make_async_copy(dy, dx_h, io.at[0]).wait()


def place_rows(ref):
    return ref.shape[1]


def backward(mesh, dy, dyt, a0, xt, a1, h1t, wg, wu, wd):
    nr, ns = mesh.shape["r"], mesh.shape["s"]
    nx = ns // 2
    tokens, d = dy.shape
    layers, nb = wg.shape[:2]
    hidden = nb * BLOCK
    m, share = d // ns, hidden // ns
    dma = pltpu.SemaphoreType.DMA
    vmem = lambda *shape, dtype=BF16: pltpu.VMEM(shape, dtype)
    up = jax.ShapeDtypeStruct((layers, m, hidden), BF16)
    return pl.pallas_call(
        functools.partial(backward_kernel, nr, ns),
        out_shape=(jax.ShapeDtypeStruct((tokens, d), BF16), up, up, jax.ShapeDtypeStruct((layers, share, d), BF16)),
        in_specs=[ANY] * 9,
        out_specs=(ANY,) * 4,
        scratch_shapes=[
            vmem(tokens, d), vmem(d, tokens), vmem(tokens, d), vmem(d, tokens), vmem(d, tokens), vmem(d, tokens, dtype=F32),
            vmem(tokens, BLOCK), vmem(tokens, BLOCK), vmem(tokens, BLOCK),
            vmem(2, d, BLOCK), vmem(2, d, BLOCK), vmem(2, BLOCK, d),
            vmem(3, 2, d, BLOCK), vmem(3, BLOCK, d),
            vmem(3, nx, 2, m, BLOCK), vmem(3, nx, 64, d),
            vmem(2, 2, 2, m, BLOCK // 2), vmem(2, 2, 32, d),
            vmem(2, 2, 2, m, BLOCK), vmem(2, 2, 64, d),
            vmem(2, nr - 1, 2, m, LANES), vmem(2, nr - 1, 16, d),
            vmem(2, 2, m, LANES), vmem(2, 16, d),
            dma((3,)), dma((3,)), dma((2,)), dma((2, 2)), dma((2,)), dma((2, 2)), dma((2,)), dma((2, 3)), dma((2,)), dma((2,)), dma((2,)),
            dma((1,)), dma((1,)), dma((5,)), dma((2, 6)),
        ],
        compiler_params=pltpu.CompilerParams(collective_id=1, has_side_effects=True, vmem_limit_bytes=VMEM_LIMIT),
        name="backward",
    )(dy, dyt, a0, xt, a1, h1t, wg, wu, wd)


def solution(mesh):
    def step(x, dy, *weights):
        a0, xt, dyt, a1, h1t, wg, wu, wd = forward(mesh, x[0], dy[0], *weights)
        dx, gg, gu, gd = backward(mesh, dy[0], dyt, a0, xt, a1, h1t, wg, wu, wd)
        return dx[None], gg, gu, gd

    states, cut = P(("rep", "r", "s"), None, None), P(None, "s", None)
    return jax.shard_map(
        step,
        mesh=mesh,
        in_specs=(states, states) + (cut,) * 3,
        out_specs=(states,) + (P("rep", "s", None),) * 3,
        check_vma=False,
    )
```

```python
import functools

import jax
import jax.numpy as jnp
from jax import lax
from jax.experimental import pallas as pl
from jax.experimental.pallas import tpu as pltpu
from jax.sharding import PartitionSpec as P

F32 = jnp.float32
BF16 = jnp.bfloat16
ANY = pl.BlockSpec(memory_space=pl.ANY)
MESH = pl.DeviceIdType.MESH
BLOCK = 512
LANES = 128
VMEM_LIMIT = 67_000_000
HOPS = (1, -1)
CORES = PAIR = range(2)
QUARTERS = 4
SMALL, BIG = 256, 1024
ALL = slice(None)
COLUMNS = [slice(n, n + SMALL) for n in range(0, BLOCK, SMALL)]
PARTS = [slice(n, n + BLOCK) for n in range(0, BIG, BLOCK)]


def dot(a, b):
    return lax.dot_general(a, b, (((1,), (0,)), ((), ())), preferred_element_type=F32)


def dot_t(a, b):
    return lax.dot_general(a, b, (((1,), (1,)), ((), ())), preferred_element_type=F32)


def rows_of(start, size):
    return pl.ds(pl.multiple_of(start, 16), size)


def lanes_of(start, size):
    return pl.ds(pl.multiple_of(start, LANES), size)


def wait_for(ref, sem):
    pltpu.make_async_copy(ref, ref, sem).wait()


class Place:
    def __init__(self, nr, ns):
        self.nr, self.nx = nr, ns // 2
        self.r, self.s = lax.axis_index("r"), lax.axis_index("s")
        self.x, self.c = self.s // 2, self.s % 2

    def at(self, dx=0, dy=0, dc=0):
        return {"r": (self.r + dy) % self.nr, "s": 2 * ((self.x + dx) % self.nx) + (self.c + dc) % 2}

    def row(self, dx):
        return 2 * ((self.x + dx) % self.nx) + self.c


def odd(n):
    return n % 2


def slot3(n):
    return n % 3


def units(ref, m, n):
    for blocks in (1, 2, 3):
        for lanes in (QUARTERS, 3, 1):
            rows, left = divmod(n, blocks * lanes)
            if not left and rows * m <= ref.shape[1]:
                return ref.at[:blocks, : m * rows, : LANES * lanes]
    raise ValueError(n)


def copies(pairs, sems):
    return [pltpu.make_async_copy(a, b, sems.at[n]) for n, (a, b) in enumerate(pairs)]


def start(things):
    for thing in things:
        thing.start()


def wait(things):
    for thing in things:
        thing.wait()


def send(src, dst, send_sem, recv_sem, device):
    pltpu.make_async_remote_copy(src_ref=src, dst_ref=dst, send_sem=send_sem, recv_sem=recv_sem, device_id=device, device_id_type=MESH).start()


def greet(peers):
    barrier = pltpu.get_barrier_semaphore()
    for peer in peers:
        pl.semaphore_signal(barrier, inc=1, device_id=peer, device_id_type=MESH)
    pl.semaphore_wait(barrier, len(peers))


class Gather:
    def __init__(self, place, whole, shard_rows, down_rows, sems):
        self.p, self.m, self.dr = place, shard_rows, down_rows
        self.up, self.down = whole
        self.nb = self.up.shape[1]
        self.x1s, self.x1r, self.x2s, self.x2r, self.ys, self.yr, self.ds, self.dr_, self.loc = sems
        self.half = place.r % 2
        self.qr = down_rows // self.nb // QUARTERS

    def piece(self, i):
        n = i % self.nb
        return i // self.nb, 4 * (odd(n)) + n // 2, n

    def rows(self, n, s, q):
        return self.qr * (QUARTERS * ((n + odd(s)) % self.nb) + q)

    def src(self, own, i, q, n):
        layer, j, t = self.piece(i)
        width = self.nb * LANES
        for e in range(n):
            yield own[0].at[layer, :, :, lanes_of(width * (q + e) + LANES * j, LANES)]
        yield own[1].at[layer, rows_of(self.rows(t, self.p.s, q), n * self.qr), :]

    def dst(self, i, s, q, n, split=False):
        layer, j, t = self.piece(i)
        rows = rows_of(self.m * s, self.m)
        if split:
            for e in range(n):
                yield self.up.at[layer, j, :, rows, lanes_of(LANES * (q + e), LANES)]
        else:
            yield self.up.at[layer, j, :, rows, lanes_of(LANES * q, n * LANES)]
        yield self.down.at[layer, rows_of(self.dr * s + self.rows(t, s, q), n * self.qr), :]

    def units(self, n):
        return units(self.up.at[0, :, 0], self.m, n)

    def own(self, own, i):
        for a, b in zip(self.src(own, i, 0, QUARTERS), self.dst(i, self.p.s, 0, QUARTERS, True)):
            send(a, b, self.x1s.at[i], self.dr_.at[i], self.p.at(dc=1))
            pltpu.make_async_copy(a, b, self.loc.at[i]).start()

    def first(self, i, own=None):
        for d, dx in enumerate(HOPS):
            there = list(self.dst(i, self.p.s, 2 * self.half, 2, own is not None))
            here = there if own is None else self.src(own, i, 2 * self.half, 2)
            for a, b in zip(here, there):
                send(a, b, self.x1s.at[i], self.x1r.at[i, d], self.p.at(dx=dx))

    def second(self, i):
        for d, dx in enumerate(HOPS):
            wait_for(self.units(6), self.x1r.at[i, d])
            for a in self.dst(i, self.p.row(-dx), 2 * self.half + d, 1):
                send(a, a, self.x2s.at[i], self.x2r.at[i, d], self.p.at(dx=dx))
        self.along(i, HOPS)

    def along(self, i, hops):
        for dx in hops:
            for d, dy in enumerate(HOPS):
                for a in self.dst(i, self.p.row(dx), 2 * self.half + d, 1):
                    send(a, a, self.ys.at[i], self.yr.at[i, d], self.p.at(dy=dy))

    def across(self, i, q, n):
        for dx in (*HOPS, 2):
            for a in self.dst(i, self.p.row(dx), q, n):
                send(a, a, self.ds.at[i], self.dr_.at[i], self.p.at(dc=1))

    def third(self, i, early=False):
        for d in PAIR:
            wait_for(self.units(3), self.x2r.at[i, d])
        self.along(i, (2,))
        if early:
            self.across(i, 2 * self.half, 2)

    def fourth(self, i, early=False):
        for d in PAIR:
            wait_for(self.units(9), self.yr.at[i, d])
        if early:
            self.across(i, 2 - 2 * self.half, 2)
        else:
            self.across(i, 0, QUARTERS)

    def sent(self, i, x1):
        for n, sem in ((x1, self.x1s), (6, self.x2s), (18, self.ys), (36, self.ds)):
            wait_for(self.units(n), sem.at[i])


def gate(g):
    sig = jnp.tanh(g * 0.5) * 0.5 + 0.5
    return sig, g * sig


def normed(h):
    return h * lax.rsqrt(jnp.mean(h * h, -1, keepdims=True) + 1e-6)


AHEAD = 2


def forward_kernel(
    nr, ns, x_h, dy_h, og_h, ou_h, od_h, xt_h, dyt_h, a0t_h, a1_h, a1t_h, h1t_h, wup_h, wd_h, f_h, act_h,
    x, y, a, t1, t2, t3, acc, act, f, oup, od, wup, wd, x1s, x1r, x2s, x2r, ys, yr, ds, dr, loc, io, wsem, fsem, asem,
):
    place = Place(nr, ns)
    tokens, d = x.shape
    layers, nb = wup_h.shape[:2]
    pieces, every = nb + AHEAD, layers * nb
    shards = lambda n: [(h.at[n], v) for h, v in ((og_h, oup.at[n, 0]), (ou_h, oup.at[n, 1]), (od_h, od.at[n]))]
    loads = shards(0) + [(x_h, x), (dy_h, y)] + shards(1)
    loads = copies(loads, io)
    start(loads)
    greet([place.at(dc=1)] + [place.at(**{dim: hop}) for dim in ("dx", "dy") for hop in HOPS])
    own = (oup, od)
    gather = Gather(place, (wup_h, wd_h), oup.shape[2], od.shape[1], (x1s, x1r, x2s, x2r, ys, yr, ds, dr, loc))

    def prepare(k, carry):
        rows = rows_of(k * SMALL, SMALL)
        h = x[rows, :]
        n = normed(h.astype(F32)).astype(BF16)
        a[rows, :] = n
        t3[:, rows] = n.T
        t1[:, rows] = h.T
        return carry

    def turn(k, carry):
        rows = rows_of(k * SMALL, SMALL)
        t2[:, rows] = y[rows, :].T
        return carry

    def begin(i):
        gather.first(i, own)
        gather.own(own, i)

    wait(loads[:3])
    begin(0)
    gather.own(own, 1)
    wait(loads[3:4])
    lax.fori_loop(0, tokens // SMALL, prepare, 0)
    gather.second(0)
    for i in (1, 2):
        gather.first(i, own)
    wait(loads[4:5])
    lax.fori_loop(0, tokens // SMALL, turn, 0)
    acc[...] = jnp.zeros_like(acc)
    wait(loads[5:])
    with jax.named_scope("third"):
        gather.third(0, True)
        gather.second(1)
        gather.first(3, own)
        gather.own(own, 2)
        gather.own(own, 3)
    outs = copies(((t1, xt_h), (t2, dyt_h), (t3, a0t_h)), io)
    with jax.named_scope("fourth"):
        gather.fourth(0, True)
    with jax.named_scope("more"):
        gather.third(1)
        gather.second(2)

    def load_up(i):
        _, j, _ = gather.piece(i)
        return pltpu.make_async_copy(wup_h.at[0, j], wup.at[odd(i)], wsem.at[odd(i), 0])

    def load_down(i):
        _, j, _ = gather.piece(i)
        return copies([(wd_h.at[0, rows_of((q * nb + j) * LANES, LANES), :], wd.at[odd(i), pl.ds(q * LANES, LANES), :]) for q in range(QUARTERS)], wsem.at[2 + odd(i)])


    def keep(i, n):
        return [pltpu.make_async_copy(f.at[n, e], f_h.at[e, i, rows_of(n * BIG, BIG), :], fsem.at[n, e]) for e in PAIR]

    def keep_act(i):
        return pltpu.make_async_copy(act.at[odd(i)], act_h.at[i], asem.at[odd(i)])

    def up(i, between):
        slot = odd(i)
        load_up(i).wait()

        @pl.when(i >= 1)
        def _():
            start((*keep(i - 1, 1), keep_act(i - 1)))

        @pl.when(i >= 2)
        def _():
            keep_act(i - 2).wait()

        def chunk(n, carry):
            @pl.when(i >= 1)
            def _():
                wait(keep(i - 1, n))

            for part in PARTS:
                rows, here = rows_of(n * BIG + part.start, BLOCK), slice(part.start, part.stop)
                for cols in COLUMNS:
                    g = dot(a[rows, :], wup[slot, 0, :, cols])
                    u = dot(a[rows, :], wup[slot, 1, :, cols])
                    sig, s = gate(g)
                    act[slot, rows, cols] = (s * u).astype(BF16)
                    f[n, 0, here, cols] = s
                    f[n, 1, here, cols] = u * (sig + s - s * sig)

            @pl.when(n == 0)
            def _():
                start(keep(i, n))
                between()

            return carry

        lax.fori_loop(0, tokens // BIG, chunk, 0)

    def down(i):
        wait(load_down(i))

        def chunk(n, carry):
            rows = rows_of(n * BIG, BIG)
            acc[rows, :] += dot(act[odd(i), rows, :], wd[odd(i)])
            return carry

        lax.fori_loop(0, tokens // BIG, chunk, 0)

    def ready(i):
        wait_for(gather.units(48), dr.at[i])
        wait_for(gather.units(12), loc.at[i])

    with jax.named_scope("ready"):
        ready(0)
    load_up(0).start()
    last = pieces - 2

    def step(i, carry):
        def between():
            with jax.named_scope("gather"):
                for n, run in enumerate((gather.fourth, gather.third, gather.second, begin), 1):

                    @pl.when(i + n <= last)
                    def _():
                        run(i + n)

                    @pl.when(i + n == last)
                    def _():
                        run(last + 1)

                @pl.when(pieces + i < every)
                def _():
                    gather.own(own, pieces + i)

        with jax.named_scope("up"):
            up(i, between)

        @pl.when(i + 1 < nb)
        def _():
            with jax.named_scope("ready"):
                ready(i + 1)
            load_up(i + 1).start()

        start(load_down(i))
        for n, out in enumerate(outs, 2):

            @pl.when(i == n)
            def _(out=out):
                out.start()

        @pl.when(i >= 1)
        def _():
            with jax.named_scope("down"):
                down(i - 1)

        return carry

    lax.fori_loop(0, nb, step, 0)
    wait((*outs, *load_down(nb - 1)))
    start((*keep(nb - 1, 1), keep_act(nb - 1)))
    finals = ((a, a1_h, 0), (t3, a1t_h, 1), (t1, h1t_h, 1))

    def finish(k, carry):
        for e in PAIR:
            rows = rows_of((2 * k + e) * SMALL, SMALL)
            y = acc[rows, :] + dot(act[(nb - 1) % 2, rows, :], wd[(nb - 1) % 2])
            h = (x[rows, :].astype(F32) + y.astype(BF16).astype(F32)).astype(BF16)
            n = normed(h.astype(F32)).astype(BF16)
            a[rows, :] = n
            t3[:, rows] = n.T
            t1[:, rows] = h.T
        rows = rows_of(2 * k * SMALL, 2 * SMALL)
        for n, (p, q, dim) in enumerate(finals):
            part = (ALL,) * dim + (rows,)
            pltpu.make_async_copy(p.at[part], q.at[part], io.at[n]).start()
        return carry

    with jax.named_scope("finish"):
        lax.fori_loop(0, tokens // SMALL // 2, finish, 0)
    for i in range(nb, pieces):
        ready(i)

    def drain(i, carry):
        gather.sent(i, 24)
        return carry

    lax.fori_loop(0, pieces, drain, 0)

    def drain_own(i, carry):
        for sem in (x1s, dr, loc):
            wait_for(gather.units(12), sem.at[i])
        return carry

    lax.fori_loop(pieces, every, drain_own, 0)
    for n in PAIR:
        wait((*keep(nb - 1, n), keep_act(nb - 1 - n)))
    wait(copies([pair[:2] for pair in finals], io))


def array(*shape, dtype=BF16):
    return jax.ShapeDtypeStruct(shape, dtype)


def vmem(*shape, dtype=BF16):
    return pltpu.VMEM(shape, dtype)


def sems(*shapes):
    return [pltpu.SemaphoreType.DMA(shape if isinstance(shape, tuple) else (shape,)) for shape in shapes]


def gather_sems(n):
    return sems(n, (n, 2), n, (n, 2), n, (n, 2), n, n, n)


def call(kernel, mesh, name, ident, outs, scratch, args, aliases={}):
    return pl.pallas_call(
        functools.partial(kernel, mesh.shape["r"], mesh.shape["s"]),
        out_shape=outs,
        in_specs=[ANY] * len(args),
        out_specs=(ANY,) * len(outs),
        input_output_aliases=aliases,
        scratch_shapes=scratch,
        compiler_params=pltpu.CompilerParams(collective_id=ident, has_side_effects=ident is not None, vmem_limit_bytes=VMEM_LIMIT),
        name=name,
    )(*args)


def forward(mesh, x, dy, w_gate, w_up, w_down):
    tokens, d = x.shape
    layers, m, hidden = w_gate.shape
    nb = hidden // BLOCK
    states, turned = array(tokens, d), array(d, tokens)
    outs = (turned, turned, turned, states, turned, turned, array(layers, nb, 2, d, BLOCK), array(layers, hidden, d), array(2, nb, tokens, BLOCK, dtype=F32), array(nb, tokens, BLOCK))
    scratch = [
        *[vmem(tokens, d)] * 3, *[vmem(d, tokens)] * 3, vmem(tokens, d, dtype=F32), vmem(2, tokens, BLOCK), vmem(2, 2, BIG, BLOCK, dtype=F32),
        vmem(layers, 2, m, hidden), vmem(*w_down.shape), vmem(2, 2, d, BLOCK), vmem(2, BLOCK, d),
        *gather_sems(layers * nb), *sems(8, (QUARTERS, QUARTERS), (2, 2), 2),
    ]
    return call(forward_kernel, mesh, "forward", 0, outs, scratch, (x, dy, w_gate, w_up, w_down))


class Reduce:
    def __init__(self, place, like, nb, layers, bufs, outs, sems):
        self.p, self.like, self.nb, self.layers = place, like, nb, layers
        self.tu, self.td, self.pu, self.pd, self.h1u, self.h1d, self.h2u, self.h2d, self.su, self.sd, self.fu, self.fd = bufs
        self.out_up, self.out_down = outs
        self.ps, self.pr, self.h1s, self.h1r, self.h2s, self.h2r, self.ss, self.sr, self.fs, self.fl, self.fx, self.ru, self.rd = sems
        self.m, self.rows = self.pu.shape[3], self.pd.shape[2]

    def own_rows(self, x, c):
        return rows_of(self.m * (2 * x + c), self.m)

    def down_rows(self, x, c):
        return rows_of(self.rows * (2 * x + c), self.rows)

    def at_x(self, dx):
        return (self.p.x + dx) % self.p.nx

    def wait(self, n, sem):
        wait_for(units(self.like, self.m, n), sem)

    def pair_up(self, b, k):
        slot, other = slot3(b), 1 - self.p.c
        for x in range(self.p.nx):
            send(self.tu.at[slot, k, self.own_rows(x, other), :], self.pu.at[slot, x, k], self.ps.at[slot], self.pr.at[slot], self.p.at(dc=1))

    def pair_down(self, b):
        slot, other = slot3(b), 1 - self.p.c
        for x in range(self.p.nx):
            send(self.td.at[slot, self.down_rows(x, other), :], self.pd.at[slot, x], self.ps.at[slot], self.pr.at[slot], self.p.at(dc=1))

    def cut(self, n, parts):
        return lanes_of(BLOCK // parts * n, BLOCK // parts), rows_of(self.rows // parts * n, self.rows // parts)

    def both(self, b, x, n, parts):
        slot = slot3(b)
        cols, rows = self.cut(n, parts)
        mine = rows_of(self.rows * (2 * x + self.p.c) + self.rows // parts * n, self.rows // parts)
        up = self.tu[slot, :, self.own_rows(x, self.p.c), cols].astype(F32) + self.pu[slot, x, :, :, cols].astype(F32)
        return up, self.td[slot, mine, :].astype(F32) + self.pd[slot, x, rows, :].astype(F32)

    def ship(self, b, x, n, parts, sums, to, send_sem, recv_sem, device):
        slot = slot3(b)
        cols, rows = self.cut(n, parts)
        refs = self.pu.at[slot, x, :, :, cols], self.pd.at[slot, x, rows, :]
        for ref, value in zip(refs, sums):
            ref[...] = value.astype(BF16)
        for ref, there in zip(refs, to):
            send(ref, there, send_sem, recv_sem, device)

    def hop(self, b, d, n, sums):
        slot = slot3(b)
        cols, rows = self.cut(n, 2)
        to = self.h2u.at[slot, d, :, :, cols], self.h2d.at[slot, d, rows, :]
        self.ship(b, self.at_x(HOPS[d]), n, 2, sums, to, self.h2s.at[slot], self.h2r.at[slot, d], self.p.at(dx=HOPS[d]))

    def first(self, b):
        slot, two = slot3(b), odd(b)
        self.wait(48, self.ps.at[slot])
        self.wait(48, self.pr.at[slot])
        x = self.at_x(2)
        for d, dx in enumerate(HOPS):
            to = self.h1u.at[two, d], self.h1d.at[two, d]
            self.ship(b, x, d, 2, self.both(b, x, d, 2), to, self.h1s.at[two], self.h1r.at[two, d], self.p.at(dx=dx))
        for d, dx in enumerate(HOPS):
            self.hop(b, d, 1 - d, self.both(b, self.at_x(dx), 1 - d, 2))

    def second(self, b):
        two = odd(b)
        for d in PAIR:
            self.wait(6, self.h1r.at[two, d])
        for d, dx in enumerate(HOPS):
            up, down = self.both(b, self.at_x(dx), d, 2)
            self.hop(b, d, d, (up + self.h1u[two, d].astype(F32), down + self.h1d[two, d].astype(F32)))

    def chip_sum(self, b, q):
        slot = slot3(b)
        cols, rows = self.cut(q, QUARTERS)
        up, down = self.both(b, self.p.x, q, QUARTERS)
        for d in PAIR:
            up, down = up + self.h2u[slot, d, :, :, cols].astype(F32), down + self.h2d[slot, d, rows, :].astype(F32)
        return up, down

    def third(self, b):
        slot, two = slot3(b), odd(b)
        self.wait(12, self.h1s.at[two])
        self.wait(24, self.h2s.at[slot])
        for d in PAIR:
            self.wait(12, self.h2r.at[slot, d])
        for n in range(self.p.nr - 1):
            q = (self.p.r + n + 1) % self.p.nr
            to = self.su.at[two, n], self.sd.at[two, n]
            self.ship(b, self.p.x, q, QUARTERS, self.chip_sum(b, q), to, self.ss.at[two], self.sr.at[two, n], self.p.at(dy=n + 1))

    def fourth(self, b):
        two = odd(b)
        layer, n = self.layers - 1 - b // self.nb, b % self.nb
        j = 4 * (odd(n)) + n // 2
        self.wait(9, self.ss.at[two])
        for n in range(self.p.nr - 1):
            self.wait(3, self.sr.at[two, n])

        @pl.when(b >= 2)
        def _():
            self.final_sent(two)

        q = self.p.r
        up, down = self.chip_sum(b, q)
        for n in range(self.p.nr - 1):
            up, down = up + self.su[two, n].astype(F32), down + self.sd[two, n].astype(F32)
        self.fu[two] = up.astype(BF16)
        self.fd[two] = down.astype(BF16)

        up_to = self.out_up.at[:, layer, :, lanes_of(LANES * (self.nb * q + j), LANES)]
        share = self.out_down.shape[1]
        first = self.rows * (2 * j + self.p.c)
        owner = first // share
        quarter = self.rows // QUARTERS
        down_to = self.out_down.at[layer, rows_of(first + quarter * q - share * owner, quarter), :]
        for dy in range(1, self.p.nr):
            send(self.fu.at[two], up_to, self.fs.at[two], self.ru.at[0], self.p.at(dy=dy))
            peer = {"r": (self.p.r + dy) % self.p.nr, "s": 2 * self.p.x + owner}
            send(self.fd.at[two], down_to, self.fs.at[two], self.rd.at[0], peer)
        pltpu.make_async_copy(self.fu.at[two], up_to, self.fl.at[two]).start()

        @pl.when(owner == self.p.c)
        def _():
            pltpu.make_async_copy(self.fd.at[two], down_to, self.fx.at[two]).start()

        @pl.when(owner != self.p.c)
        def _():
            send(self.fd.at[two], down_to, self.fx.at[two], self.rd.at[0], self.p.at(dc=1))

    def final_sent(self, two):
        for n, sem in ((9, self.fs), (2, self.fl), (1, self.fx)):
            self.wait(n, sem.at[two])


def backward_kernel(
    nr, ns, dy_h, dyt_h, a0t_h, xt_h, a1_h, a1t_h, h1t_h, f_h, act_h, wup_in, wd_in, dx_h, gup_h, gd_h, wup_h, wd_h, kept_h,
    a, at, dy, dyt, ht, dat, f, act, dg, du, wup, wd, tu, td, pu, pd, h1u, h1d, h2u, h2d, su, sd, fu, fd,
    ps, pr, h1s, h1r, h2s, h2r, ss, sr, fs, fl, fx, ru, rd, x1s, x1r, x2s, x2r, ys, yr, ds, dr, _, io, wsem, ksem, fsem,
):
    place = Place(nr, ns)
    tokens, d = a.shape
    layers, nb = wup_h.shape[:2]
    steps = layers * nb
    loads = copies(((a1_h, a), (dy_h, dy), (a1t_h, at), (dyt_h, dyt), (h1t_h, ht)), io)
    gather = Gather(place, (wup_h, wd_h), gup_h.shape[2], gd_h.shape[1], (x1s, x1r, x2s, x2r, ys, yr, ds, dr, None))
    ahead = nb + AHEAD

    def block_of(b):
        return gather.piece(steps - nb + b % nb - (b // nb) * nb)

    def load_up(b):
        layer, j, _ = block_of(b)
        return pltpu.make_async_copy(wup_h.at[layer, j], wup.at[odd(b)], wsem.at[odd(b), 0])

    def load_down(b):
        layer, j, _ = block_of(b)
        return copies([(wd_h.at[layer, rows_of((q * nb + j) * LANES, LANES), :], wd.at[odd(b), pl.ds(q * LANES, LANES), :]) for q in range(QUARTERS)], wsem.at[2 + odd(b)])

    start((*loads[:2], load_up(0), *load_down(0)))
    greet([place.at(dc=1)] + [place.at(dx=hop) for hop in HOPS] + [place.at(dy=hop, dc=c) for hop in range(1, nr) for c in CORES])
    reduce = Reduce(
        place, wup_h.at[0, :, 0], nb, layers, (tu, td, pu, pd, h1u, h1d, h2u, h2d, su, sd, fu, fd), (gup_h, gd_h),
        (ps, pr, h1s, h1r, h2s, h2r, ss, sr, fs, fl, fx, ru, rd),
    )
    dat[...] = jnp.zeros_like(dat)
    wait(loads[:2])
    start(loads[2:])

    def layer_end(begin, end, last):
        def chunk(n, carry):
            cols = lanes_of(n * SMALL, SMALL)

            def part(rows):
                return ht[rows, cols].astype(F32), dat[rows, cols].astype(BF16).astype(F32)

            def sums(i, so_far):
                h, da = part(rows_of(i * LANES, LANES))
                return tuple(s + jnp.sum((v * h).reshape(-1, 8, SMALL), 0) for s, v in zip(so_far, (h, da)))

            none = jnp.zeros((8, SMALL), F32)
            square, cross = (jnp.sum(v, 0, keepdims=True) for v in lax.fori_loop(0, d // LANES, sums, (none, none)))
            scale = lax.rsqrt(square / d + 1e-6)
            h, da = part(ALL)
            v = dyt[:, cols].astype(F32) + scale * (da - h * scale * (scale * cross / d))
            v = v.astype(BF16)
            if not last:
                dyt[:, cols] = v
                dat[:, cols] = jnp.zeros((d, SMALL), F32)
            dy[cols, :] = v.T
            return carry

        with jax.named_scope("end"):
            lax.fori_loop(begin // SMALL, end // SMALL, chunk, 0)

    def keep(k):
        return copies([(v, kept_h.at[n, k - nb]) for n, v in enumerate((dg, du))], ksem)

    def load_f(q):
        rows = rows_of(q % QUARTERS * BLOCK, BLOCK)
        return copies([(f_h.at[e, q // QUARTERS, rows, :], f.at[slot3(q), e]) for e in PAIR], fsem.at[slot3(q)])

    def load_act(k):
        return pltpu.make_async_copy(act_h.at[k - nb], act, ksem.at[2])

    def compute(k, between):
        slot = odd(k)
        wait((load_up(k), *load_down(k)))

        def chunk(n, carry):
            for part in PARTS:
                rows = rows_of(n * BIG + part.start, BLOCK)
                for cols in COLUMNS:
                    g = dot(a[rows, :], wup[slot, 0, :, cols])
                    u = dot(a[rows, :], wup[slot, 1, :, cols])
                    e = dot_t(dy[rows, :], wd[slot, cols, :]).astype(BF16).astype(F32)
                    sig, s = gate(g)
                    act[rows, cols] = (s * u).astype(BF16)
                    dg[rows, cols] = (e * u * (sig + s - s * sig)).astype(BF16)
                    du[rows, cols] = (e * s).astype(BF16)

            @pl.when(n == 0)
            def _():
                between()

            return carry

        lax.fori_loop(0, tokens // BIG, chunk, 0)

    def compute_last(k):
        slot = odd(k)
        wait((load_up(k), *load_down(k)))

        @pl.when(k > nb)
        def _():
            wait(keep(k - 1))

        def chunk(n, carry):
            q = (k - nb) * QUARTERS + n
            wait(load_f(q))

            @pl.when(q + 2 < nb * QUARTERS)
            def _():
                start(load_f(q + 2))

            for cols in COLUMNS:
                e = dot_t(dy[rows_of(n * BLOCK, BLOCK), :], wd[slot, cols, :]).astype(BF16).astype(F32)
                for n_, v in enumerate((du, dg)):
                    v[rows_of(n * BLOCK, BLOCK), cols] = (e * f[slot3(q), n_, :, cols]).astype(BF16)
            return carry

        lax.fori_loop(0, tokens // BLOCK, chunk, 0)
        @pl.when(k < steps - 1)
        def _():
            start(keep(k))

    def terms(k, n, before=None):
        slot = slot3(k)
        if n < 2:
            for cols in (slice(0, SMALL), slice(SMALL, BLOCK)):
                tu[slot, n, :, cols] = dot(at[...], (dg, du)[n][:, cols]).astype(BF16)
            reduce.pair_up(k, n)
        else:
            @pl.when(k >= nb)
            def _():
                load_act(k).wait()

            for cols in (slice(0, SMALL), slice(SMALL, BLOCK)):
                td[slot, cols, :] = dot(dyt[...], act[:, cols]).astype(BF16).T
            before()
            reduce.pair_down(k)

    def back(k):
        slot = odd(k)
        for n in range(tokens // BLOCK):
            cols = pl.ds(n * BLOCK, BLOCK)
            dat[:, cols] += dot_t(wup[slot, 0], dg[cols, :]) + dot_t(wup[slot, 1], du[cols, :])

    def back_half(half, slot, first):
        rows, cols = rows_of(first, BIG), lanes_of(half * BIG, BIG)
        dat[:, cols] += dot_t(wup[slot, 0], dg[rows, :]) + dot_t(wup[slot, 1], du[rows, :])

    def later(t):
        half = jnp.where(t == 2, 0, 1)
        j = jnp.where(t == 2, nb - 2, t - 3)
        _, order, _ = gather.piece(j)
        slot = odd(t)
        yield pltpu.make_async_copy(wup_h.at[0, order], wup.at[slot], wsem.at[slot, 0])
        for n, v in enumerate((dg, du), 1):
            yield pltpu.make_async_copy(kept_h.at[n - 1, j, rows_of(half * BIG, BIG), :], v.at[rows_of(slot * BIG, BIG), :], wsem.at[slot, n])

    def back_later(t):
        @pl.when(t >= 2)
        def _():
            wait(later(t))

        @pl.when((t >= 1) & (t < nb + 1))
        def _():
            start(later(t + 1))

        slot = odd(t)
        back_half(jnp.where((t == 0) | (t == 2), 0, 1), jnp.where(t == 0, 1, slot), slot * BIG)

    def done(half):
        rows = pl.ds(half * BIG, BIG)
        return pltpu.make_async_copy(dy.at[rows, :], dx_h.at[rows, :], io.at[half])

    def step(k, carry):
        t = k - steps

        def stage(run, lag, *late):
            b = k - lag
            now = (k >= lag) & (k < steps)
            for n, when in enumerate(late):
                now = now | (t == when)
                b = jnp.where(t == when, steps - len(late) + n, b)

            @pl.when(now)
            def _():
                with jax.named_scope("r_" + run.__name__):
                    run(b)

        def tick(*entries):
            for group, when, run in entries:

                @pl.when(k == when)
                def _():
                    with jax.named_scope(f"gather_{group}_{when}"):
                        for i in (range(ahead, ahead + 2), range(ahead + 2, steps))[group]:
                            run(i)

        def arrived(i):
            wait_for(gather.units(36), dr.at[i])

        tick((0, 0, gather.first), (1, 3, gather.fourth))

        def between():
            stage(reduce.third, 2)

        @pl.when(k < nb)
        def _():
            with jax.named_scope("compute"):
                compute(k, between)

        @pl.when((k >= nb) & (k < steps))
        def _():
            with jax.named_scope("compute_last"):
                compute_last(k)

        tick((0, 0, gather.second), (0, 1, gather.fourth), (1, 1, gather.second), (1, 2, gather.third))

        @pl.when((k >= nb - 1) & (k + 1 < steps))
        def _():
            start((load_up(k + 1), *load_down(k + 1)))

        @pl.when(k >= nb)
        def _():
            stage(reduce.third, 2, 2, 5)

        stage(reduce.first, 1, 1)

        @pl.when(k == 0)
        def _():
            wait(loads[2:])

        def terms_of(n, before=None):
            @pl.when(k < steps)
            def _():
                with jax.named_scope(f"terms_{n}"):
                    terms(k, n, before)

        terms_of(0)
        terms_of(1)
        terms_of(2, lambda: stage(reduce.fourth, 2))

        @pl.when(k >= steps)
        def _():
            stage(reduce.fourth, steps, 4, nb)

        stage(reduce.second, 1, 3)
        tick((0, 0, gather.third), (1, 0, gather.first), (0, 1, arrived), (1, 3, arrived))

        @pl.when((k >= nb - 1) & (k + 1 < steps))
        def _():
            load_act(k + 1).start()

        @pl.when(k < nb - 1)
        def _():
            start((load_up(k + 1), *load_down(k + 1)))

        @pl.when(k < nb)
        def _():
            with jax.named_scope("back"):
                back(k)

        @pl.when((k >= nb) & (k < steps - 2))
        def _():
            with jax.named_scope("back_half"):
                back_half(0, odd(k), 0)

        @pl.when(k == nb - 1)
        def _():
            load = pltpu.make_async_copy(a0t_h, at, io.at[0])
            start((load, *load_f(0), *load_f(1)))
            layer_end(0, tokens, False)
            turned.start()
            load.wait()

        @pl.when((t >= 0) & (t < nb + 2))
        def _():
            with jax.named_scope("back_later"):
                back_later(t)

        @pl.when(t == 2)
        def _():
            turned.wait()
            layer_end(0, BIG, True)
            done(0).start()

        return carry

    turned = pltpu.make_async_copy(xt_h, ht, io.at[4])
    lax.fori_loop(0, steps + nb + 2, step, 0)
    layer_end(BIG, tokens, True)
    done(1).start()

    def drain(i, carry):
        gather.sent(i, 12)
        return carry

    lax.fori_loop(ahead, steps, drain, 0)
    for two in PAIR:
        reduce.final_sent(two)
    reduce.wait(6 * steps, ru.at[0])
    reduce.wait(48, rd.at[0])
    wait((done(0), done(1)))


def backward(mesh, dy, dyt, a0t, xt, a1, a1t, h1t, f, act, wup, wd):
    nr, ns = mesh.shape["r"], mesh.shape["s"]
    nx = ns // 2
    tokens, d = dy.shape
    layers, nb = wup.shape[:2]
    hidden = nb * BLOCK
    m, share, rows = d // ns, hidden // ns, BLOCK // ns
    outs = (array(tokens, d), array(2, layers, m, hidden), array(layers, share, d), array(*wup.shape), array(*wd.shape), array(2, nb, tokens, BLOCK))
    scratch = [
        *[vmem(tokens, d), vmem(d, tokens)] * 2, vmem(d, tokens), vmem(d, tokens, dtype=F32), vmem(3, 2, BLOCK, BLOCK, dtype=F32), *[vmem(tokens, BLOCK)] * 3,
        vmem(2, 2, d, BLOCK), vmem(2, BLOCK, d), vmem(3, 2, d, BLOCK), vmem(3, BLOCK, d), vmem(3, nx, 2, m, BLOCK), vmem(3, nx, rows, d),
        vmem(2, 2, 2, m, BLOCK // 2), vmem(2, 2, rows // 2, d), vmem(3, 2, 2, m, BLOCK), vmem(3, 2, rows, d),
        vmem(2, nr - 1, 2, m, LANES), vmem(2, nr - 1, rows // QUARTERS, d), vmem(2, 2, m, LANES), vmem(2, rows // QUARTERS, d),
        *sems(3, 3, 2, (2, 2), 3, (3, 2), 2, (2, nr - 1), 2, 2, 2, 1, 1), *gather_sems(layers * nb), *sems(5, (QUARTERS, QUARTERS), 3, (3, 2)),
    ]
    return call(backward_kernel, mesh, "backward", 1, outs, scratch, (dy, dyt, a0t, xt, a1, a1t, h1t, f, act, wup, wd), {9: 3, 10: 4})[:3]


def deliver_kernel(nr, ns, dx_h, gup_h, gd_h, out_x, out_gate, out_up, out_down, x, up, down, arrive, leave):
    jobs = []
    for h, out, v in ((dx_h, out_x, x), (gup_h.at[0], out_gate, up.at[0]), (gup_h.at[1], out_up, up.at[1]), (gd_h, out_down, down)):
        size = BIG if out is out_x else 1
        for n in range(0, out.shape[0], size):
            part = pl.ds(n, size)
            jobs.append((h.at[part], v.at[part], out.at[part]))
    loads = copies([job[:2] for job in jobs], arrive)
    stores = copies([job[1:] for job in jobs], leave)
    start(loads)
    for load, store in zip(loads, stores):
        load.wait()
        store.start()
    wait(stores)


def deliver(mesh, dx, gup, gd):
    up = gup.shape[1:]
    scratch = [vmem(*v.shape) for v in (dx, gup, gd)] + sems(8, 8)
    return call(deliver_kernel, mesh, "deliver", None, (array(*dx.shape), array(*up), array(*up), array(*gd.shape)), scratch, (dx, gup, gd))


def solution(mesh):
    def step(x, dy, *weights):
        xt, dyt, a0t, a1, a1t, h1t, wup, wd, f, act = forward(mesh, x[0], dy[0], *weights)
        results = backward(mesh, dy[0], dyt, a0t, xt, a1, a1t, h1t, f, act, wup, wd)
        dx, *by_weights = deliver(mesh, *results)
        return dx[None], *by_weights

    states, cut = P(("rep", "r", "s"), None, None), P(None, "s", None)
    return jax.shard_map(
        step,
        mesh=mesh,
        in_specs=(states, states) + (cut,) * 3,
        out_specs=(states,) + (P("rep", "s", None),) * 3,
        check_vma=False,
    )
```

```python
import functools

import jax
import jax.numpy as jnp
from jax import lax
from jax.experimental import pallas as pl
from jax.experimental.pallas import tpu as pltpu
from jax.sharding import PartitionSpec as P

F32 = jnp.float32
BF16 = jnp.bfloat16
ANY = pl.BlockSpec(memory_space=pl.ANY)
MESH = pl.DeviceIdType.MESH
BLOCK = 512
LANES = 128
VMEM_LIMIT = 67_000_000
HOPS = (1, -1)
CORES = PAIR = range(2)
QUARTERS = 4
SMALL, BIG = 256, 1024
ALL = slice(None)
COLUMNS = [slice(n, n + SMALL) for n in range(0, BLOCK, SMALL)]
PARTS = [slice(n, n + BLOCK) for n in range(0, BIG, BLOCK)]


def dot(a, b):
    return lax.dot_general(a, b, (((1,), (0,)), ((), ())), preferred_element_type=F32)


def dot_t(a, b):
    return lax.dot_general(a, b, (((1,), (1,)), ((), ())), preferred_element_type=F32)


def rows_of(start, size):
    return pl.ds(pl.multiple_of(start, 16), size)


def lanes_of(start, size):
    return pl.ds(pl.multiple_of(start, LANES), size)


def wait_for(ref, sem):
    pltpu.make_async_copy(ref, ref, sem).wait()


class Place:
    def __init__(self, nr, ns):
        self.nr, self.nx = nr, ns // 2
        self.r, self.s = lax.axis_index("r"), lax.axis_index("s")
        self.x, self.c = self.s // 2, self.s % 2

    def at(self, dx=0, dy=0, dc=0):
        return {"r": (self.r + dy) % self.nr, "s": 2 * ((self.x + dx) % self.nx) + (self.c + dc) % 2}

    def row(self, dx):
        return 2 * ((self.x + dx) % self.nx) + self.c


def odd(n):
    return n % 2


def slot3(n):
    return n % 3


def units(ref, m, n):
    for blocks in (1, 2, 3):
        for lanes in (QUARTERS, 3, 1):
            rows, left = divmod(n, blocks * lanes)
            if not left and rows * m <= ref.shape[1]:
                return ref.at[:blocks, : m * rows, : LANES * lanes]
    raise ValueError(n)


def copies(pairs, sems):
    return [pltpu.make_async_copy(a, b, sems.at[n]) for n, (a, b) in enumerate(pairs)]


def start(things):
    for thing in things:
        thing.start()


def wait(things):
    for thing in things:
        thing.wait()


def send(src, dst, send_sem, recv_sem, device):
    pltpu.make_async_remote_copy(src_ref=src, dst_ref=dst, send_sem=send_sem, recv_sem=recv_sem, device_id=device, device_id_type=MESH).start()


def greet(peers):
    barrier = pltpu.get_barrier_semaphore()
    for peer in peers:
        pl.semaphore_signal(barrier, inc=1, device_id=peer, device_id_type=MESH)
    pl.semaphore_wait(barrier, len(peers))


class Gather:
    def __init__(self, place, whole, shard_rows, down_rows, sems):
        self.p, self.m, self.dr = place, shard_rows, down_rows
        self.up, self.down = whole
        self.nb = self.up.shape[1]
        self.x1s, self.x1r, self.x2s, self.x2r, self.ys, self.yr, self.ds, self.dr_, self.loc = sems
        self.half = place.r % 2
        self.qr = down_rows // self.nb // QUARTERS

    def piece(self, i):
        n = i % self.nb
        return i // self.nb, 4 * (odd(n)) + n // 2, n

    def rows(self, n, s, q):
        return self.qr * (QUARTERS * ((n + odd(s)) % self.nb) + q)

    def src(self, own, i, q, n):
        layer, j, t = self.piece(i)
        width = self.nb * LANES
        for e in range(n):
            yield own[0].at[layer, :, :, lanes_of(width * (q + e) + LANES * j, LANES)]
        yield own[1].at[layer, rows_of(self.rows(t, self.p.s, q), n * self.qr), :]

    def dst(self, i, s, q, n, split=False):
        layer, j, t = self.piece(i)
        rows = rows_of(self.m * s, self.m)
        if split:
            for e in range(n):
                yield self.up.at[layer, j, :, rows, lanes_of(LANES * (q + e), LANES)]
        else:
            yield self.up.at[layer, j, :, rows, lanes_of(LANES * q, n * LANES)]
        yield self.down.at[layer, rows_of(self.dr * s + self.rows(t, s, q), n * self.qr), :]

    def units(self, n):
        return units(self.up.at[0, :, 0], self.m, n)

    def own(self, own, i):
        for a, b in zip(self.src(own, i, 0, QUARTERS), self.dst(i, self.p.s, 0, QUARTERS, True)):
            send(a, b, self.x1s.at[i], self.dr_.at[i], self.p.at(dc=1))
            pltpu.make_async_copy(a, b, self.loc.at[i]).start()

    def first(self, i, own=None):
        for d, dx in enumerate(HOPS):
            there = list(self.dst(i, self.p.s, 2 * self.half, 2, own is not None))
            here = there if own is None else self.src(own, i, 2 * self.half, 2)
            for a, b in zip(here, there):
                send(a, b, self.x1s.at[i], self.x1r.at[i, d], self.p.at(dx=dx))

    def second(self, i):
        for d, dx in enumerate(HOPS):
            wait_for(self.units(6), self.x1r.at[i, d])
            for a in self.dst(i, self.p.row(-dx), 2 * self.half + d, 1):
                send(a, a, self.x2s.at[i], self.x2r.at[i, d], self.p.at(dx=dx))
        self.along(i, HOPS)

    def along(self, i, hops):
        for dx in hops:
            for d, dy in enumerate(HOPS):
                for a in self.dst(i, self.p.row(dx), 2 * self.half + d, 1):
                    send(a, a, self.ys.at[i], self.yr.at[i, d], self.p.at(dy=dy))

    def across(self, i, q, n):
        for dx in (*HOPS, 2):
            for a in self.dst(i, self.p.row(dx), q, n):
                send(a, a, self.ds.at[i], self.dr_.at[i], self.p.at(dc=1))

    def third(self, i, early=False):
        for d in PAIR:
            wait_for(self.units(3), self.x2r.at[i, d])
        self.along(i, (2,))
        if early:
            self.across(i, 2 * self.half, 2)

    def fourth(self, i, early=False):
        for d in PAIR:
            wait_for(self.units(9), self.yr.at[i, d])
        if early:
            self.across(i, 2 - 2 * self.half, 2)
        else:
            self.across(i, 0, QUARTERS)

    def sent(self, i, x1):
        for n, sem in ((x1, self.x1s), (6, self.x2s), (18, self.ys), (36, self.ds)):
            wait_for(self.units(n), sem.at[i])


def gate(g):
    sig = jnp.tanh(g * 0.5) * 0.5 + 0.5
    return sig, g * sig


def normed(h):
    return h * lax.rsqrt(jnp.mean(h * h, -1, keepdims=True) + 1e-6)


AHEAD = 2


def forward_kernel(
    nr, ns, x_h, dy_h, og_h, ou_h, od_h, xt_h, dyt_h, a0t_h, a1_h, a1t_h, h1t_h, wup_h, wd_h, f_h, act_h,
    x, y, a, t1, t2, t3, acc, act, f, oup, od, wup, wd, x1s, x1r, x2s, x2r, ys, yr, ds, dr, loc, io, wsem, fsem, asem,
):
    place = Place(nr, ns)
    tokens, d = x.shape
    layers, nb = wup_h.shape[:2]
    pieces, every = nb + AHEAD, layers * nb
    shards = lambda n: [(h.at[n], v) for h, v in ((og_h, oup.at[n, 0]), (ou_h, oup.at[n, 1]), (od_h, od.at[n]))]
    loads = shards(0) + [(x_h, x), (dy_h, y)] + shards(1)
    loads = copies(loads, io)
    start(loads)
    greet([place.at(dc=1)] + [place.at(**{dim: hop}) for dim in ("dx", "dy") for hop in HOPS])
    own = (oup, od)
    gather = Gather(place, (wup_h, wd_h), oup.shape[2], od.shape[1], (x1s, x1r, x2s, x2r, ys, yr, ds, dr, loc))

    def norm_rows(rows, h):
        n = normed(h.astype(F32)).astype(BF16)
        a[rows, :] = n
        t3[:, rows] = n.T
        t1[:, rows] = h.T

    def prepare(k, carry):
        rows = rows_of(k * SMALL, SMALL)
        norm_rows(rows, x[rows, :])
        return carry

    def turn(k, carry):
        rows = rows_of(k * SMALL, SMALL)
        t2[:, rows] = y[rows, :].T
        return carry

    def begin(i):
        gather.first(i, own)
        gather.own(own, i)

    wait(loads[:3])
    begin(0)
    gather.own(own, 1)
    wait(loads[3:4])
    lax.fori_loop(0, tokens // SMALL, prepare, 0)
    gather.second(0)
    for i in (1, 2):
        gather.first(i, own)
    wait(loads[4:5])
    lax.fori_loop(0, tokens // SMALL, turn, 0)
    acc[...] = jnp.zeros_like(acc)
    wait(loads[5:])
    with jax.named_scope("third"):
        gather.third(0, True)
        gather.second(1)
        gather.first(3, own)
        gather.own(own, 2)
        gather.own(own, 3)
    outs = copies(((t1, xt_h), (t2, dyt_h), (t3, a0t_h)), io)
    with jax.named_scope("fourth"):
        gather.fourth(0, True)
    with jax.named_scope("more"):
        gather.third(1)
        gather.second(2)

    def load_up(i):
        _, j, _ = gather.piece(i)
        return pltpu.make_async_copy(wup_h.at[0, j], wup.at[odd(i)], wsem.at[odd(i), 0])

    def load_down(i):
        _, j, _ = gather.piece(i)
        return copies([(wd_h.at[0, rows_of((q * nb + j) * LANES, LANES), :], wd.at[odd(i), pl.ds(q * LANES, LANES), :]) for q in range(QUARTERS)], wsem.at[2 + odd(i)])


    def keep(i, n):
        return [pltpu.make_async_copy(f.at[n, e], f_h.at[e, i, rows_of(n * BIG, BIG), :], fsem.at[n, e]) for e in PAIR]

    def keep_act(i):
        return pltpu.make_async_copy(act.at[odd(i)], act_h.at[i], asem.at[odd(i)])

    def up(i, between):
        slot = odd(i)
        load_up(i).wait()

        @pl.when(i >= 1)
        def _():
            start((*keep(i - 1, 1), keep_act(i - 1)))

        @pl.when(i >= 2)
        def _():
            keep_act(i - 2).wait()

        def chunk(n, carry):
            @pl.when(i >= 1)
            def _():
                wait(keep(i - 1, n))

            for part in PARTS:
                rows, here = rows_of(n * BIG + part.start, BLOCK), slice(part.start, part.stop)
                for cols in COLUMNS:
                    g = dot(a[rows, :], wup[slot, 0, :, cols])
                    u = dot(a[rows, :], wup[slot, 1, :, cols])
                    sig, s = gate(g)
                    act[slot, rows, cols] = (s * u).astype(BF16)
                    f[n, 0, here, cols] = s
                    f[n, 1, here, cols] = u * (sig + s - s * sig)

            @pl.when(n == 0)
            def _():
                start(keep(i, n))
                between()

            return carry

        lax.fori_loop(0, tokens // BIG, chunk, 0)

    def down(i):
        wait(load_down(i))

        def chunk(n, carry):
            rows = rows_of(n * BIG, BIG)
            acc[rows, :] += dot(act[odd(i), rows, :], wd[odd(i)])
            return carry

        lax.fori_loop(0, tokens // BIG, chunk, 0)

    def ready(i):
        wait_for(gather.units(48), dr.at[i])
        wait_for(gather.units(12), loc.at[i])

    with jax.named_scope("ready"):
        ready(0)
    load_up(0).start()
    def step(i, carry):
        def between():
            with jax.named_scope("gather"):
                for n, run in enumerate((gather.fourth, gather.third, gather.second, begin), 1):

                    @pl.when(i + n < pieces)
                    def _():
                        run(i + n)

                @pl.when(pieces + i < every)
                def _():
                    gather.own(own, pieces + i)

        with jax.named_scope("up"):
            up(i, between)

        @pl.when(i + 1 < nb)
        def _():
            with jax.named_scope("ready"):
                ready(i + 1)
            load_up(i + 1).start()

        start(load_down(i))
        for n, out in enumerate(outs, 2):

            @pl.when(i == n)
            def _(out=out):
                out.start()

        @pl.when(i >= 1)
        def _():
            with jax.named_scope("down"):
                down(i - 1)

        return carry

    lax.fori_loop(0, nb, step, 0)
    gather.fourth(pieces - 1)
    wait((*outs, *load_down(nb - 1)))
    start((*keep(nb - 1, 1), keep_act(nb - 1)))
    finals = ((a, a1_h, 0), (t3, a1t_h, 1), (t1, h1t_h, 1))

    def finish(k, carry):
        for e in PAIR:
            rows = rows_of((2 * k + e) * SMALL, SMALL)
            y = acc[rows, :] + dot(act[(nb - 1) % 2, rows, :], wd[(nb - 1) % 2])
            norm_rows(rows, (x[rows, :].astype(F32) + y.astype(BF16).astype(F32)).astype(BF16))
        rows = rows_of(2 * k * SMALL, 2 * SMALL)
        for n, (p, q, dim) in enumerate(finals):
            part = (ALL,) * dim + (rows,)
            pltpu.make_async_copy(p.at[part], q.at[part], io.at[n]).start()
        return carry

    with jax.named_scope("finish"):
        lax.fori_loop(0, tokens // SMALL // 2, finish, 0)
    for i in range(nb, pieces):
        ready(i)

    def drain(i, carry):
        gather.sent(i, 24)
        return carry

    lax.fori_loop(0, pieces, drain, 0)

    def drain_own(i, carry):
        for sem in (x1s, dr, loc):
            wait_for(gather.units(12), sem.at[i])
        return carry

    lax.fori_loop(pieces, every, drain_own, 0)
    for n in PAIR:
        wait((*keep(nb - 1, n), keep_act(nb - 1 - n)))
    wait(copies([pair[:2] for pair in finals], io))


def array(*shape, dtype=BF16):
    return jax.ShapeDtypeStruct(shape, dtype)


def vmem(*shape, dtype=BF16):
    return pltpu.VMEM(shape, dtype)


def sems(*shapes):
    return [pltpu.SemaphoreType.DMA(shape if isinstance(shape, tuple) else (shape,)) for shape in shapes]


def gather_sems(n):
    return sems(n, (n, 2), n, (n, 2), n, (n, 2), n, n, n)


def call(kernel, mesh, name, ident, outs, scratch, args, aliases={}):
    return pl.pallas_call(
        functools.partial(kernel, mesh.shape["r"], mesh.shape["s"]),
        out_shape=outs,
        in_specs=[ANY] * len(args),
        out_specs=(ANY,) * len(outs),
        input_output_aliases=aliases,
        scratch_shapes=scratch,
        compiler_params=pltpu.CompilerParams(collective_id=ident, has_side_effects=ident is not None, vmem_limit_bytes=VMEM_LIMIT),
        name=name,
    )(*args)


def forward(mesh, x, dy, w_gate, w_up, w_down):
    tokens, d = x.shape
    layers, m, hidden = w_gate.shape
    nb = hidden // BLOCK
    states, turned = array(tokens, d), array(d, tokens)
    outs = (turned, turned, turned, states, turned, turned, array(layers, nb, 2, d, BLOCK), array(layers, hidden, d), array(2, nb, tokens, BLOCK, dtype=F32), array(nb, tokens, BLOCK))
    scratch = [
        *[vmem(tokens, d)] * 3, *[vmem(d, tokens)] * 3, vmem(tokens, d, dtype=F32), vmem(2, tokens, BLOCK), vmem(2, 2, BIG, BLOCK, dtype=F32),
        vmem(layers, 2, m, hidden), vmem(*w_down.shape), vmem(2, 2, d, BLOCK), vmem(2, BLOCK, d),
        *gather_sems(layers * nb), *sems(8, (QUARTERS, QUARTERS), (2, 2), 2),
    ]
    return call(forward_kernel, mesh, "forward", 0, outs, scratch, (x, dy, w_gate, w_up, w_down))


class Reduce:
    def __init__(self, place, like, nb, layers, bufs, outs, sems):
        self.p, self.like, self.nb, self.layers = place, like, nb, layers
        self.tu, self.td, self.pu, self.pd, self.h1u, self.h1d, self.h2u, self.h2d, self.su, self.sd, self.fu, self.fd = bufs
        self.out_up, self.out_down = outs
        self.ps, self.pr, self.h1s, self.h1r, self.h2s, self.h2r, self.ss, self.sr, self.fs, self.fl, self.fx, self.ru, self.rd = sems
        self.m, self.rows = self.pu.shape[3], self.pd.shape[2]

    def own_rows(self, x, c):
        return rows_of(self.m * (2 * x + c), self.m)

    def down_rows(self, x, c):
        return rows_of(self.rows * (2 * x + c), self.rows)

    def at_x(self, dx):
        return (self.p.x + dx) % self.p.nx

    def wait(self, n, sem):
        wait_for(units(self.like, self.m, n), sem)

    def pair_up(self, b):
        slot, other = slot3(b), 1 - self.p.c
        for x in range(self.p.nx):
            send(self.tu.at[slot, :, self.own_rows(x, other), :], self.pu.at[slot, x], self.ps.at[slot], self.pr.at[slot], self.p.at(dc=1))

    def pair_down(self, b):
        slot, other = slot3(b), 1 - self.p.c
        for x in range(self.p.nx):
            send(self.td.at[slot, self.down_rows(x, other), :], self.pd.at[slot, x], self.ps.at[slot], self.pr.at[slot], self.p.at(dc=1))

    def cut(self, n, parts):
        return lanes_of(BLOCK // parts * n, BLOCK // parts), rows_of(self.rows // parts * n, self.rows // parts)

    def both(self, b, x, n, parts):
        slot = slot3(b)
        cols, rows = self.cut(n, parts)
        mine = rows_of(self.rows * (2 * x + self.p.c) + self.rows // parts * n, self.rows // parts)
        up = self.tu[slot, :, self.own_rows(x, self.p.c), cols].astype(F32) + self.pu[slot, x, :, :, cols].astype(F32)
        return up, self.td[slot, mine, :].astype(F32) + self.pd[slot, x, rows, :].astype(F32)

    def ship(self, b, x, n, parts, sums, to, send_sem, recv_sem, device):
        slot = slot3(b)
        cols, rows = self.cut(n, parts)
        refs = self.pu.at[slot, x, :, :, cols], self.pd.at[slot, x, rows, :]
        for ref, value in zip(refs, sums):
            ref[...] = value.astype(BF16)
        for ref, there in zip(refs, to):
            send(ref, there, send_sem, recv_sem, device)

    def hop(self, b, d, n, sums):
        slot = slot3(b)
        cols, rows = self.cut(n, 2)
        to = self.h2u.at[slot, d, :, :, cols], self.h2d.at[slot, d, rows, :]
        self.ship(b, self.at_x(HOPS[d]), n, 2, sums, to, self.h2s.at[slot], self.h2r.at[slot, d], self.p.at(dx=HOPS[d]))

    def first(self, b):
        slot, two = slot3(b), odd(b)
        self.wait(48, self.ps.at[slot])
        self.wait(48, self.pr.at[slot])
        x = self.at_x(2)
        for d, dx in enumerate(HOPS):
            to = self.h1u.at[two, d], self.h1d.at[two, d]
            self.ship(b, x, d, 2, self.both(b, x, d, 2), to, self.h1s.at[two], self.h1r.at[two, d], self.p.at(dx=dx))
        for d, dx in enumerate(HOPS):
            self.hop(b, d, 1 - d, self.both(b, self.at_x(dx), 1 - d, 2))

    def second(self, b):
        two = odd(b)
        for d in PAIR:
            self.wait(6, self.h1r.at[two, d])
        for d, dx in enumerate(HOPS):
            up, down = self.both(b, self.at_x(dx), d, 2)
            self.hop(b, d, d, (up + self.h1u[two, d].astype(F32), down + self.h1d[two, d].astype(F32)))

    def chip_sum(self, b, q):
        slot = slot3(b)
        cols, rows = self.cut(q, QUARTERS)
        up, down = self.both(b, self.p.x, q, QUARTERS)
        for d in PAIR:
            up, down = up + self.h2u[slot, d, :, :, cols].astype(F32), down + self.h2d[slot, d, rows, :].astype(F32)
        return up, down

    def third(self, b):
        slot, two = slot3(b), odd(b)
        self.wait(12, self.h1s.at[two])
        self.wait(24, self.h2s.at[slot])
        for d in PAIR:
            self.wait(12, self.h2r.at[slot, d])
        for n in range(self.p.nr - 1):
            q = (self.p.r + n + 1) % self.p.nr
            to = self.su.at[two, n], self.sd.at[two, n]
            self.ship(b, self.p.x, q, QUARTERS, self.chip_sum(b, q), to, self.ss.at[two], self.sr.at[two, n], self.p.at(dy=n + 1))

    def fourth(self, b):
        two = odd(b)
        layer, n = self.layers - 1 - b // self.nb, b % self.nb
        j = 4 * (odd(n)) + n // 2
        self.wait(9, self.ss.at[two])
        for n in range(self.p.nr - 1):
            self.wait(3, self.sr.at[two, n])

        @pl.when(b >= 2)
        def _():
            self.final_sent(two)

        q = self.p.r
        up, down = self.chip_sum(b, q)
        for n in range(self.p.nr - 1):
            up, down = up + self.su[two, n].astype(F32), down + self.sd[two, n].astype(F32)
        self.fu[two] = up.astype(BF16)
        self.fd[two] = down.astype(BF16)

        up_to = self.out_up.at[:, layer, :, lanes_of(LANES * (self.nb * q + j), LANES)]
        share = self.out_down.shape[1]
        first = self.rows * (2 * j + self.p.c)
        owner = first // share
        quarter = self.rows // QUARTERS
        down_to = self.out_down.at[layer, rows_of(first + quarter * q - share * owner, quarter), :]
        for dy in range(1, self.p.nr):
            send(self.fu.at[two], up_to, self.fs.at[two], self.ru.at[0], self.p.at(dy=dy))
            peer = {"r": (self.p.r + dy) % self.p.nr, "s": 2 * self.p.x + owner}
            send(self.fd.at[two], down_to, self.fs.at[two], self.rd.at[0], peer)
        pltpu.make_async_copy(self.fu.at[two], up_to, self.fl.at[two]).start()

        @pl.when(owner == self.p.c)
        def _():
            pltpu.make_async_copy(self.fd.at[two], down_to, self.fx.at[two]).start()

        @pl.when(owner != self.p.c)
        def _():
            send(self.fd.at[two], down_to, self.fx.at[two], self.rd.at[0], self.p.at(dc=1))

    def final_sent(self, two):
        for n, sem in ((9, self.fs), (2, self.fl), (1, self.fx)):
            self.wait(n, sem.at[two])


def backward_kernel(
    nr, ns, dy_h, dyt_h, a0t_h, xt_h, a1_h, a1t_h, h1t_h, f_h, act_h, wup_in, wd_in, dx_h, gup_h, gd_h, wup_h, wd_h, kept_h,
    a, at, dy, dyt, ht, dat, f, act, dg, du, wup, wd, tu, td, pu, pd, h1u, h1d, h2u, h2d, su, sd, fu, fd,
    ps, pr, h1s, h1r, h2s, h2r, ss, sr, fs, fl, fx, ru, rd, x1s, x1r, x2s, x2r, ys, yr, ds, dr, _, io, wsem, ksem, fsem,
):
    place = Place(nr, ns)
    tokens, d = a.shape
    layers, nb = wup_h.shape[:2]
    steps = layers * nb
    halves = [(h.at[pl.ds(n, BIG), :], v.at[pl.ds(n, BIG), :]) for n in range(0, tokens, BIG) for h, v in ((a1_h, a), (dy_h, dy))]
    loads = copies(halves + [(a1t_h, at), (dyt_h, dyt), (h1t_h, ht)], io)
    gather = Gather(place, (wup_h, wd_h), gup_h.shape[2], gd_h.shape[1], (x1s, x1r, x2s, x2r, ys, yr, ds, dr, None))
    ahead = nb + AHEAD

    def block_of(b):
        return gather.piece(steps - nb + b % nb - (b // nb) * nb)

    def load_up(b):
        layer, j, _ = block_of(b)
        return pltpu.make_async_copy(wup_h.at[layer, j], wup.at[odd(b)], wsem.at[odd(b), 0])

    def load_down(b):
        layer, j, _ = block_of(b)
        return copies([(wd_h.at[layer, rows_of((q * nb + j) * LANES, LANES), :], wd.at[odd(b), pl.ds(q * LANES, LANES), :]) for q in range(QUARTERS)], wsem.at[2 + odd(b)])

    start((*loads[:2], load_up(0), *load_down(0), *loads[2:4]))
    greet([place.at(dc=1)] + [place.at(dx=hop) for hop in HOPS] + [place.at(dy=hop, dc=c) for hop in range(1, nr) for c in CORES])
    reduce = Reduce(
        place, wup_h.at[0, :, 0], nb, layers, (tu, td, pu, pd, h1u, h1d, h2u, h2d, su, sd, fu, fd), (gup_h, gd_h),
        (ps, pr, h1s, h1r, h2s, h2r, ss, sr, fs, fl, fx, ru, rd),
    )
    dat[...] = jnp.zeros_like(dat)
    wait(loads[:2])

    def layer_end(begin, end, last):
        def chunk(n, carry):
            cols = lanes_of(n * SMALL, SMALL)

            def part(rows):
                return ht[rows, cols].astype(F32), dat[rows, cols].astype(BF16).astype(F32)

            def sums(i, so_far):
                h, da = part(rows_of(i * LANES, LANES))
                return tuple(s + jnp.sum((v * h).reshape(-1, 8, SMALL), 0) for s, v in zip(so_far, (h, da)))

            none = jnp.zeros((8, SMALL), F32)
            square, cross = (jnp.sum(v, 0, keepdims=True) for v in lax.fori_loop(0, d // LANES, sums, (none, none)))
            scale = lax.rsqrt(square / d + 1e-6)
            h, da = part(ALL)
            v = dyt[:, cols].astype(F32) + scale * (da - h * scale * (scale * cross / d))
            v = v.astype(BF16)
            if not last:
                dyt[:, cols] = v
                dat[:, cols] = jnp.zeros((d, SMALL), F32)
            dy[cols, :] = v.T
            return carry

        with jax.named_scope("end"):
            lax.fori_loop(begin // SMALL, end // SMALL, chunk, 0)

    def keep(k):
        return copies([(v, kept_h.at[n, k - nb]) for n, v in enumerate((dg, du))], ksem)

    def load_f(q):
        rows = rows_of(q % QUARTERS * BLOCK, BLOCK)
        return copies([(f_h.at[e, q // QUARTERS, rows, :], f.at[slot3(q), e]) for e in PAIR], fsem.at[slot3(q)])

    def load_act(k):
        return pltpu.make_async_copy(act_h.at[k - nb], act, ksem.at[2])

    def compute(k, between):
        slot = odd(k)
        wait((load_up(k), *load_down(k)))

        def chunk(n, carry):
            for part in PARTS:
                rows = rows_of(n * BIG + part.start, BLOCK)
                for cols in COLUMNS:
                    g = dot(a[rows, :], wup[slot, 0, :, cols])
                    u = dot(a[rows, :], wup[slot, 1, :, cols])
                    e = dot_t(dy[rows, :], wd[slot, cols, :]).astype(BF16).astype(F32)
                    sig, s = gate(g)
                    act[rows, cols] = (s * u).astype(BF16)
                    dg[rows, cols] = (e * u * (sig + s - s * sig)).astype(BF16)
                    du[rows, cols] = (e * s).astype(BF16)

            @pl.when(n == 0)
            def _():
                between()

            return carry

        lax.fori_loop(0, tokens // BIG, chunk, 0)

    def compute_last(k):
        slot = odd(k)
        wait((load_up(k), *load_down(k)))

        @pl.when(k > nb)
        def _():
            wait(keep(k - 1))

        def chunk(n, carry):
            q = (k - nb) * QUARTERS + n
            wait(load_f(q))

            @pl.when(q + 2 < nb * QUARTERS)
            def _():
                start(load_f(q + 2))

            for cols in COLUMNS:
                e = dot_t(dy[rows_of(n * BLOCK, BLOCK), :], wd[slot, cols, :]).astype(BF16).astype(F32)
                for n_, v in enumerate((du, dg)):
                    v[rows_of(n * BLOCK, BLOCK), cols] = (e * f[slot3(q), n_, :, cols]).astype(BF16)
            return carry

        lax.fori_loop(0, tokens // BLOCK, chunk, 0)
        @pl.when(k < steps - 1)
        def _():
            start(keep(k))

    def terms(k, before):
        slot = slot3(k)

        @pl.when(k >= nb)
        def _():
            load_act(k).wait()

        for cols in COLUMNS:
            td[slot, cols, :] = dot(dyt[...], act[:, cols]).astype(BF16).T
        for n, left in enumerate((dg, du)):
            for cols in COLUMNS:
                tu[slot, n, :, cols] = dot(at[...], left[:, cols]).astype(BF16)
        reduce.pair_up(k)
        before()
        reduce.pair_down(k)

    def back(k):
        slot = odd(k)
        for n in range(tokens // BLOCK):
            cols = pl.ds(n * BLOCK, BLOCK)
            dat[:, cols] += dot_t(wup[slot, 0], dg[cols, :]) + dot_t(wup[slot, 1], du[cols, :])

    def back_half(half, slot, first):
        rows, cols = rows_of(first, BIG), lanes_of(half * BIG, BIG)
        dat[:, cols] += dot_t(wup[slot, 0], dg[rows, :]) + dot_t(wup[slot, 1], du[rows, :])

    def later(t):
        half = jnp.where(t == 2, 0, 1)
        j = jnp.where(t == 2, nb - 2, t - 3)
        _, order, _ = gather.piece(j)
        slot = odd(t)
        yield pltpu.make_async_copy(wup_h.at[0, order], wup.at[slot], wsem.at[slot, 0])
        for n, v in enumerate((dg, du), 1):
            yield pltpu.make_async_copy(kept_h.at[n - 1, j, rows_of(half * BIG, BIG), :], v.at[rows_of(slot * BIG, BIG), :], wsem.at[slot, n])

    def back_later(t):
        @pl.when(t >= 2)
        def _():
            wait(later(t))

        @pl.when((t >= 1) & (t < nb + 1))
        def _():
            start(later(t + 1))

        slot = odd(t)
        back_half(jnp.where((t == 0) | (t == 2), 0, 1), jnp.where(t == 0, 1, slot), slot * BIG)

    def done(half):
        rows = pl.ds(half * BIG, BIG)
        return pltpu.make_async_copy(dy.at[rows, :], dx_h.at[rows, :], io.at[half])

    def step(k, carry):
        t = k - steps

        def stage(run, lag, *late):
            b = k - lag
            now = (k >= lag) & (k < steps)
            for n, when in enumerate(late):
                now = now | (t == when)
                b = jnp.where(t == when, steps - len(late) + n, b)

            @pl.when(now)
            def _():
                with jax.named_scope("r_" + run.__name__):
                    run(b)

        def tick(*entries):
            for pieces, when, run in entries:

                @pl.when(k == when)
                def _():
                    with jax.named_scope("gather"):
                        for i in pieces:
                            run(ahead + i)

        one, two, rest = (0,), (1,), range(2, steps - ahead)

        def arrived(i):
            wait_for(gather.units(36), dr.at[i])

        tick((one, 0, gather.first), (two, 0, gather.first), (one, 1, gather.fourth), (two, 1, gather.third), (rest, 3, gather.fourth))

        def between():
            @pl.when(k == 0)
            def _():
                wait(loads[2:4])
                start(loads[4:])

            stage(reduce.third, 2)

        @pl.when(k < nb)
        def _():
            with jax.named_scope("compute"):
                compute(k, between)

        @pl.when((k >= nb) & (k < steps))
        def _():
            with jax.named_scope("compute_last"):
                compute_last(k)

        tick((one, 0, gather.second), (two, 1, gather.fourth), (rest, 2, gather.third))

        @pl.when((k >= nb - 1) & (k + 1 < steps))
        def _():
            start((load_up(k + 1), *load_down(k + 1)))

        @pl.when(k >= nb)
        def _():
            stage(reduce.third, 2, 2, 5)

        stage(reduce.first, 1, 1)

        @pl.when(k == 0)
        def _():
            wait(loads[4:])

        @pl.when(k < steps)
        def _():
            with jax.named_scope("terms"):
                terms(k, lambda: stage(reduce.fourth, 2))

        @pl.when(k >= steps)
        def _():
            stage(reduce.fourth, steps, 4, nb)

        stage(reduce.second, 1, 3)
        tick((one, 0, gather.third), (two, 0, gather.second), (rest, 0, gather.first), ((0, 1), 1, arrived), (rest, 1, gather.second), (rest, 3, arrived))

        @pl.when((k >= nb - 1) & (k + 1 < steps))
        def _():
            load_act(k + 1).start()

        @pl.when(k < nb - 1)
        def _():
            start((load_up(k + 1), *load_down(k + 1)))

        @pl.when(k < nb)
        def _():
            with jax.named_scope("back"):
                back(k)

        @pl.when((k >= nb) & (k < steps - 2))
        def _():
            with jax.named_scope("back_half"):
                back_half(0, odd(k), 0)

        @pl.when(k == nb - 1)
        def _():
            load = pltpu.make_async_copy(a0t_h, at, io.at[0])
            start((load, *load_f(0), *load_f(1)))
            layer_end(0, tokens, False)
            turned.start()
            load.wait()

        @pl.when((t >= 0) & (t < nb + 2))
        def _():
            with jax.named_scope("back_later"):
                back_later(t)

        @pl.when(t == 2)
        def _():
            turned.wait()
            layer_end(0, BIG, True)
            done(0).start()

        return carry

    turned = pltpu.make_async_copy(xt_h, ht, io.at[4])
    lax.fori_loop(0, steps + nb + 2, step, 0)
    layer_end(BIG, tokens, True)
    done(1).start()

    def drain(i, carry):
        gather.sent(i, 12)
        return carry

    lax.fori_loop(ahead, steps, drain, 0)
    for two in PAIR:
        reduce.final_sent(two)
    reduce.wait(6 * steps, ru.at[0])
    reduce.wait(48, rd.at[0])
    wait((done(0), done(1)))


def backward(mesh, dy, dyt, a0t, xt, a1, a1t, h1t, f, act, wup, wd):
    nr, ns = mesh.shape["r"], mesh.shape["s"]
    nx = ns // 2
    tokens, d = dy.shape
    layers, nb = wup.shape[:2]
    hidden = nb * BLOCK
    m, share, rows = d // ns, hidden // ns, BLOCK // ns
    outs = (array(tokens, d), array(2, layers, m, hidden), array(layers, share, d), array(*wup.shape), array(*wd.shape), array(2, nb, tokens, BLOCK))
    scratch = [
        *[vmem(tokens, d), vmem(d, tokens)] * 2, vmem(d, tokens), vmem(d, tokens, dtype=F32), vmem(3, 2, BLOCK, BLOCK, dtype=F32), *[vmem(tokens, BLOCK)] * 3,
        vmem(2, 2, d, BLOCK), vmem(2, BLOCK, d), vmem(3, 2, d, BLOCK), vmem(3, BLOCK, d), vmem(3, nx, 2, m, BLOCK), vmem(3, nx, rows, d),
        vmem(2, 2, 2, m, BLOCK // 2), vmem(2, 2, rows // 2, d), vmem(3, 2, 2, m, BLOCK), vmem(3, 2, rows, d),
        vmem(2, nr - 1, 2, m, LANES), vmem(2, nr - 1, rows // QUARTERS, d), vmem(2, 2, m, LANES), vmem(2, rows // QUARTERS, d),
        *sems(3, 3, 2, (2, 2), 3, (3, 2), 2, (2, nr - 1), 2, 2, 2, 1, 1), *gather_sems(layers * nb), *sems(8, (QUARTERS, QUARTERS), 3, (3, 2)),
    ]
    return call(backward_kernel, mesh, "backward", 1, outs, scratch, (dy, dyt, a0t, xt, a1, a1t, h1t, f, act, wup, wd), {9: 3, 10: 4})[:3]


def deliver_kernel(nr, ns, dx_h, gup_h, gd_h, out_x, out_gate, out_up, out_down, x, up, down, arrive, leave):
    jobs = []
    for h, out, v in ((dx_h, out_x, x), (gup_h.at[0], out_gate, up.at[0]), (gup_h.at[1], out_up, up.at[1]), (gd_h, out_down, down)):
        size = BIG if out is out_x else 1
        for n in range(0, out.shape[0], size):
            part = pl.ds(n, size)
            jobs.append((h.at[part], v.at[part], out.at[part]))
    loads = copies([job[:2] for job in jobs], arrive)
    stores = copies([job[1:] for job in jobs], leave)
    start(loads)
    for load, store in zip(loads, stores):
        load.wait()
        store.start()
    wait(stores)


def deliver(mesh, dx, gup, gd):
    up = gup.shape[1:]
    scratch = [vmem(*v.shape) for v in (dx, gup, gd)] + sems(8, 8)
    return call(deliver_kernel, mesh, "deliver", None, (array(*dx.shape), array(*up), array(*up), array(*gd.shape)), scratch, (dx, gup, gd))


def solution(mesh):
    def step(x, dy, *weights):
        xt, dyt, a0t, a1, a1t, h1t, wup, wd, f, act = forward(mesh, x[0], dy[0], *weights)
        results = backward(mesh, dy[0], dyt, a0t, xt, a1, a1t, h1t, f, act, wup, wd)
        dx, *by_weights = deliver(mesh, *results)
        return dx[None], *by_weights

    states, cut = P(("rep", "r", "s"), None, None), P(None, "s", None)
    return jax.shard_map(
        step,
        mesh=mesh,
        in_specs=(states, states) + (cut,) * 3,
        out_specs=(states,) + (P("rep", "s", None),) * 3,
        check_vma=False,
    )
```

```python
import functools

import jax
import jax.numpy as jnp
from jax import lax
from jax.experimental import pallas as pl
from jax.experimental.pallas import tpu as pltpu
from jax.sharding import PartitionSpec as P

F32 = jnp.float32
BF16 = jnp.bfloat16
ANY = pl.BlockSpec(memory_space=pl.ANY)
MESH = pl.DeviceIdType.MESH
BLOCK = 512
LANES = 128
VMEM_LIMIT = 67_000_000
HOPS = (1, -1)
CORES = PAIR = range(2)
QUARTERS = 4
SMALL, BIG = 256, 1024
ALL = slice(None)
COLUMNS = [slice(n, n + SMALL) for n in range(0, BLOCK, SMALL)]
PARTS = [slice(n, n + BLOCK) for n in range(0, BIG, BLOCK)]


def dot(a, b):
    return lax.dot_general(a, b, (((1,), (0,)), ((), ())), preferred_element_type=F32)


def dot_t(a, b):
    return lax.dot_general(a, b, (((1,), (1,)), ((), ())), preferred_element_type=F32)


def rows_of(start, size):
    return pl.ds(pl.multiple_of(start, 16), size)


def lanes_of(start, size):
    return pl.ds(pl.multiple_of(start, LANES), size)


def wait_for(ref, sem):
    pltpu.make_async_copy(ref, ref, sem).wait()


class Place:
    def __init__(self, nr, ns):
        self.nr, self.nx = nr, ns // 2
        self.r, self.s = lax.axis_index("r"), lax.axis_index("s")
        self.x, self.c = self.s // 2, self.s % 2

    def at(self, dx=0, dy=0, dc=0):
        return {"r": (self.r + dy) % self.nr, "s": 2 * ((self.x + dx) % self.nx) + (self.c + dc) % 2}

    def row(self, dx):
        return 2 * ((self.x + dx) % self.nx) + self.c


def odd(n):
    return n % 2


def slot3(n):
    return n % 3


def units(ref, m, n):
    for blocks in (1, 2, 3):
        for lanes in (QUARTERS, 3, 1):
            rows, left = divmod(n, blocks * lanes)
            if not left and rows * m <= ref.shape[1]:
                return ref.at[:blocks, : m * rows, : LANES * lanes]
    raise ValueError(n)


def copies(pairs, sems):
    return [pltpu.make_async_copy(a, b, sems.at[n]) for n, (a, b) in enumerate(pairs)]


def start(things):
    for thing in things:
        thing.start()


def wait(things):
    for thing in things:
        thing.wait()


def send(src, dst, send_sem, recv_sem, device):
    pltpu.make_async_remote_copy(src_ref=src, dst_ref=dst, send_sem=send_sem, recv_sem=recv_sem, device_id=device, device_id_type=MESH).start()


def greet(peers):
    barrier = pltpu.get_barrier_semaphore()
    for peer in peers:
        pl.semaphore_signal(barrier, inc=1, device_id=peer, device_id_type=MESH)
    pl.semaphore_wait(barrier, len(peers))


class Gather:
    def __init__(self, place, whole, shard_rows, down_rows, sems):
        self.p, self.m, self.dr = place, shard_rows, down_rows
        self.up, self.down = whole
        self.nb = self.up.shape[1]
        self.x1s, self.x1r, self.x2s, self.x2r, self.ys, self.yr, self.ds, self.dr_, self.loc = sems
        self.half = place.r % 2
        self.qr = down_rows // self.nb // QUARTERS

    def piece(self, i):
        n = i % self.nb
        return i // self.nb, 4 * (odd(n)) + n // 2, n

    def rows(self, n, s, q):
        return self.qr * (QUARTERS * ((n + odd(s)) % self.nb) + q)

    def src(self, own, i, q, n):
        layer, j, t = self.piece(i)
        width = self.nb * LANES
        for e in range(n):
            yield own[0].at[layer, :, :, lanes_of(width * (q + e) + LANES * j, LANES)]
        yield own[1].at[layer, rows_of(self.rows(t, self.p.s, q), n * self.qr), :]

    def dst(self, i, s, q, n, split=False):
        layer, j, t = self.piece(i)
        rows = rows_of(self.m * s, self.m)
        if split:
            for e in range(n):
                yield self.up.at[layer, j, :, rows, lanes_of(LANES * (q + e), LANES)]
        else:
            yield self.up.at[layer, j, :, rows, lanes_of(LANES * q, n * LANES)]
        yield self.down.at[layer, rows_of(self.dr * s + self.rows(t, s, q), n * self.qr), :]

    def units(self, n):
        return units(self.up.at[0, :, 0], self.m, n)

    def own(self, own, i):
        for a, b in zip(self.src(own, i, 0, QUARTERS), self.dst(i, self.p.s, 0, QUARTERS, True)):
            send(a, b, self.x1s.at[i], self.dr_.at[i], self.p.at(dc=1))
            pltpu.make_async_copy(a, b, self.loc.at[i]).start()

    def first(self, i, own=None):
        for d, dx in enumerate(HOPS):
            there = list(self.dst(i, self.p.s, 2 * self.half, 2, own is not None))
            here = there if own is None else self.src(own, i, 2 * self.half, 2)
            for a, b in zip(here, there):
                send(a, b, self.x1s.at[i], self.x1r.at[i, d], self.p.at(dx=dx))

    def second(self, i):
        for d, dx in enumerate(HOPS):
            wait_for(self.units(6), self.x1r.at[i, d])
            for a in self.dst(i, self.p.row(-dx), 2 * self.half + d, 1):
                send(a, a, self.x2s.at[i], self.x2r.at[i, d], self.p.at(dx=dx))
        self.along(i, HOPS)

    def along(self, i, hops):
        for dx in hops:
            for d, dy in enumerate(HOPS):
                for a in self.dst(i, self.p.row(dx), 2 * self.half + d, 1):
                    send(a, a, self.ys.at[i], self.yr.at[i, d], self.p.at(dy=dy))

    def across(self, i, q, n):
        for dx in (*HOPS, 2):
            for a in self.dst(i, self.p.row(dx), q, n):
                send(a, a, self.ds.at[i], self.dr_.at[i], self.p.at(dc=1))

    def third(self, i, early=False):
        for d in PAIR:
            wait_for(self.units(3), self.x2r.at[i, d])
        self.along(i, (2,))
        if early:
            self.across(i, 2 * self.half, 2)

    def fourth(self, i, early=False):
        for d in PAIR:
            wait_for(self.units(9), self.yr.at[i, d])
        if early:
            self.across(i, 2 - 2 * self.half, 2)
        else:
            self.across(i, 0, QUARTERS)

    def sent(self, i, x1):
        for n, sem in ((x1, self.x1s), (6, self.x2s), (18, self.ys), (36, self.ds)):
            wait_for(self.units(n), sem.at[i])


def gate(g):
    sig = jnp.tanh(g * 0.5) * 0.5 + 0.5
    return sig, g * sig


def normed(h):
    return h * lax.rsqrt(jnp.mean(h * h, -1, keepdims=True) + 1e-6)


AHEAD = 2


def forward_kernel(
    nr, ns, x_h, dy_h, og_h, ou_h, od_h, xt_h, dyt_h, a0t_h, a1_h, a1t_h, h1t_h, wup_h, wd_h, f_h, act_h,
    x, y, a, t1, t2, t3, acc, act, f, oup, od, wup, wd, x1s, x1r, x2s, x2r, ys, yr, ds, dr, loc, io, wsem, fsem, asem,
):
    place = Place(nr, ns)
    tokens, d = x.shape
    layers, nb = wup_h.shape[:2]
    pieces, every = nb + AHEAD, layers * nb
    shards = lambda n: [(h.at[n], v) for h, v in ((og_h, oup.at[n, 0]), (ou_h, oup.at[n, 1]), (od_h, od.at[n]))]
    loads = shards(0) + [(x_h, x), (dy_h, y)] + shards(1)
    loads = copies(loads, io)
    start(loads)
    greet([place.at(dc=1)] + [place.at(**{dim: hop}) for dim in ("dx", "dy") for hop in HOPS])
    own = (oup, od)
    gather = Gather(place, (wup_h, wd_h), oup.shape[2], od.shape[1], (x1s, x1r, x2s, x2r, ys, yr, ds, dr, loc))

    def norm_rows(rows, h):
        n = normed(h.astype(F32)).astype(BF16)
        a[rows, :] = n
        t3[:, rows] = n.T
        t1[:, rows] = h.T

    def prepare(k, carry):
        rows = rows_of(k * SMALL, SMALL)
        norm_rows(rows, x[rows, :])
        return carry

    def turn(k, carry):
        rows = rows_of(k * SMALL, SMALL)
        t2[:, rows] = y[rows, :].T
        return carry

    def begin(i):
        gather.first(i, own)
        gather.own(own, i)

    wait(loads[:3])
    begin(0)
    gather.own(own, 1)
    wait(loads[3:4])
    lax.fori_loop(0, tokens // SMALL, prepare, 0)
    gather.second(0)
    for i in (1, 2):
        gather.first(i, own)
    wait(loads[4:5])
    lax.fori_loop(0, tokens // SMALL, turn, 0)
    acc[...] = jnp.zeros_like(acc)
    wait(loads[5:])
    with jax.named_scope("third"):
        gather.third(0, True)
        gather.second(1)
        gather.first(3, own)
        gather.own(own, 2)
        gather.own(own, 3)
    outs = copies(((t1, xt_h), (t2, dyt_h), (t3, a0t_h)), io)
    with jax.named_scope("fourth"):
        gather.fourth(0, True)
    with jax.named_scope("more"):
        gather.third(1)
        gather.second(2)

    def load_up(i):
        _, j, _ = gather.piece(i)
        return pltpu.make_async_copy(wup_h.at[0, j], wup.at[odd(i)], wsem.at[odd(i), 0])

    def load_down(i):
        _, j, _ = gather.piece(i)
        return copies([(wd_h.at[0, rows_of((q * nb + j) * LANES, LANES), :], wd.at[odd(i), pl.ds(q * LANES, LANES), :]) for q in range(QUARTERS)], wsem.at[2 + odd(i)])


    def keep(i, n):
        return [pltpu.make_async_copy(f.at[n, e], f_h.at[e, i, rows_of(n * BIG, BIG), :], fsem.at[n, e]) for e in PAIR]

    def keep_act(i):
        return pltpu.make_async_copy(act.at[odd(i)], act_h.at[i], asem.at[odd(i)])

    def up(i, between):
        slot = odd(i)
        load_up(i).wait()

        @pl.when(i >= 1)
        def _():
            start((*keep(i - 1, 1), keep_act(i - 1)))

        @pl.when(i >= 2)
        def _():
            keep_act(i - 2).wait()

        def chunk(n, carry):
            @pl.when(i >= 1)
            def _():
                wait(keep(i - 1, n))

            for part in PARTS:
                rows, here = rows_of(n * BIG + part.start, BLOCK), slice(part.start, part.stop)
                for cols in COLUMNS:
                    g = dot(a[rows, :], wup[slot, 0, :, cols])
                    u = dot(a[rows, :], wup[slot, 1, :, cols])
                    sig, s = gate(g)
                    act[slot, rows, cols] = (s * u).astype(BF16)
                    f[n, 0, here, cols] = s
                    f[n, 1, here, cols] = u * (sig + s - s * sig)

            @pl.when(n == 0)
            def _():
                start(keep(i, n))
                between()

            return carry

        lax.fori_loop(0, tokens // BIG, chunk, 0)

    def down(i):
        wait(load_down(i))

        for n in range(tokens // BIG):
            rows = pl.ds(n * BIG, BIG)
            acc[rows, :] += dot(act[odd(i), rows, :], wd[odd(i)])

    def ready(i):
        wait_for(gather.units(48), dr.at[i])
        wait_for(gather.units(12), loc.at[i])

    with jax.named_scope("ready"):
        ready(0)
    load_up(0).start()
    def step(i, carry):
        def between():
            with jax.named_scope("gather"):
                for n, run in enumerate((gather.fourth, gather.third, gather.second, begin), 1):

                    @pl.when(i + n < pieces)
                    def _():
                        run(i + n)

                @pl.when(pieces + i < every)
                def _():
                    gather.own(own, pieces + i)

        with jax.named_scope("up"):
            up(i, between)

        @pl.when(i + 1 < nb)
        def _():
            with jax.named_scope("ready"):
                ready(i + 1)
            load_up(i + 1).start()

        start(load_down(i))
        for n, out in enumerate(outs, 2):

            @pl.when(i == n)
            def _(out=out):
                out.start()

        @pl.when(i >= 1)
        def _():
            with jax.named_scope("down"):
                down(i - 1)

        return carry

    lax.fori_loop(0, nb, step, 0)
    gather.fourth(pieces - 1)
    wait((*outs, *load_down(nb - 1)))
    start((*keep(nb - 1, 1), keep_act(nb - 1)))
    finals = ((a, a1_h, 0), (t3, a1t_h, 1), (t1, h1t_h, 1))

    def finish(k, carry):
        for e in PAIR:
            rows = rows_of((2 * k + e) * SMALL, SMALL)
            y = acc[rows, :] + dot(act[(nb - 1) % 2, rows, :], wd[(nb - 1) % 2])
            norm_rows(rows, (x[rows, :].astype(F32) + y.astype(BF16).astype(F32)).astype(BF16))
        rows = rows_of(2 * k * SMALL, 2 * SMALL)
        for n, (p, q, dim) in enumerate(finals):
            part = (ALL,) * dim + (rows,)
            pltpu.make_async_copy(p.at[part], q.at[part], io.at[n]).start()
        return carry

    with jax.named_scope("finish"):
        lax.fori_loop(0, tokens // SMALL // 2, finish, 0)
    for i in range(nb, pieces):
        ready(i)

    def drain(i, carry):
        gather.sent(i, 24)
        return carry

    lax.fori_loop(0, pieces, drain, 0)

    def drain_own(i, carry):
        for sem in (x1s, dr, loc):
            wait_for(gather.units(12), sem.at[i])
        return carry

    lax.fori_loop(pieces, every, drain_own, 0)
    for n in PAIR:
        wait((*keep(nb - 1, n), keep_act(nb - 1 - n)))
    wait(copies([pair[:2] for pair in finals], io))


def array(*shape, dtype=BF16):
    return jax.ShapeDtypeStruct(shape, dtype)


def vmem(*shape, dtype=BF16):
    return pltpu.VMEM(shape, dtype)


def sems(*shapes):
    return [pltpu.SemaphoreType.DMA(shape if isinstance(shape, tuple) else (shape,)) for shape in shapes]


def gather_sems(n):
    return sems(n, (n, 2), n, (n, 2), n, (n, 2), n, n, n)


def call(kernel, mesh, name, ident, outs, scratch, args, aliases={}):
    return pl.pallas_call(
        functools.partial(kernel, mesh.shape["r"], mesh.shape["s"]),
        out_shape=outs,
        in_specs=[ANY] * len(args),
        out_specs=(ANY,) * len(outs),
        input_output_aliases=aliases,
        scratch_shapes=scratch,
        compiler_params=pltpu.CompilerParams(collective_id=ident, has_side_effects=ident is not None, vmem_limit_bytes=VMEM_LIMIT),
        name=name,
    )(*args)


def forward(mesh, x, dy, w_gate, w_up, w_down):
    tokens, d = x.shape
    layers, m, hidden = w_gate.shape
    nb = hidden // BLOCK
    states, turned = array(tokens, d), array(d, tokens)
    outs = (turned, turned, turned, states, turned, turned, array(layers, nb, 2, d, BLOCK), array(layers, hidden, d), array(2, nb, tokens, BLOCK, dtype=F32), array(nb, tokens, BLOCK))
    scratch = [
        *[vmem(tokens, d)] * 3, *[vmem(d, tokens)] * 3, vmem(tokens, d, dtype=F32), vmem(2, tokens, BLOCK), vmem(2, 2, BIG, BLOCK, dtype=F32),
        vmem(layers, 2, m, hidden), vmem(*w_down.shape), vmem(2, 2, d, BLOCK), vmem(2, BLOCK, d),
        *gather_sems(layers * nb), *sems(8, (QUARTERS, QUARTERS), (2, 2), 2),
    ]
    return call(forward_kernel, mesh, "forward", 0, outs, scratch, (x, dy, w_gate, w_up, w_down))


class Reduce:
    def __init__(self, place, like, nb, layers, bufs, outs, sems):
        self.p, self.like, self.nb, self.layers = place, like, nb, layers
        self.tu, self.td, self.pu, self.pd, self.h1u, self.h1d, self.h2u, self.h2d, self.su, self.sd, self.fu, self.fd = bufs
        self.out_up, self.out_down = outs
        self.ps, self.pr, self.h1s, self.h1r, self.h2s, self.h2r, self.ss, self.sr, self.fs, self.fl, self.fx, self.ru, self.rd = sems
        self.m, self.rows = self.pu.shape[3], self.pd.shape[2]

    def own_rows(self, x, c):
        return rows_of(self.m * (2 * x + c), self.m)

    def down_rows(self, x, c):
        return rows_of(self.rows * (2 * x + c), self.rows)

    def at_x(self, dx):
        return (self.p.x + dx) % self.p.nx

    def wait(self, n, sem):
        wait_for(units(self.like, self.m, n), sem)

    def pair_up(self, b):
        slot, other = slot3(b), 1 - self.p.c
        for x in range(self.p.nx):
            send(self.tu.at[slot, :, self.own_rows(x, other), :], self.pu.at[slot, x], self.ps.at[slot], self.pr.at[slot], self.p.at(dc=1))

    def pair_down(self, b):
        slot, other = slot3(b), 1 - self.p.c
        for x in range(self.p.nx):
            send(self.td.at[slot, self.down_rows(x, other), :], self.pd.at[slot, x], self.ps.at[slot], self.pr.at[slot], self.p.at(dc=1))

    def cut(self, n, parts):
        return lanes_of(BLOCK // parts * n, BLOCK // parts), rows_of(self.rows // parts * n, self.rows // parts)

    def both(self, b, x, n, parts):
        slot = slot3(b)
        cols, rows = self.cut(n, parts)
        mine = rows_of(self.rows * (2 * x + self.p.c) + self.rows // parts * n, self.rows // parts)
        up = self.tu[slot, :, self.own_rows(x, self.p.c), cols].astype(F32) + self.pu[slot, x, :, :, cols].astype(F32)
        return up, self.td[slot, mine, :].astype(F32) + self.pd[slot, x, rows, :].astype(F32)

    def ship(self, b, x, n, parts, sums, to, send_sem, recv_sem, device):
        slot = slot3(b)
        cols, rows = self.cut(n, parts)
        refs = self.pu.at[slot, x, :, :, cols], self.pd.at[slot, x, rows, :]
        for ref, value in zip(refs, sums):
            ref[...] = value.astype(BF16)
        for ref, there in zip(refs, to):
            send(ref, there, send_sem, recv_sem, device)

    def hop(self, b, d, n, sums):
        slot = slot3(b)
        cols, rows = self.cut(n, 2)
        to = self.h2u.at[slot, d, :, :, cols], self.h2d.at[slot, d, rows, :]
        self.ship(b, self.at_x(HOPS[d]), n, 2, sums, to, self.h2s.at[slot], self.h2r.at[slot, d], self.p.at(dx=HOPS[d]))

    def first(self, b):
        slot, two = slot3(b), odd(b)
        self.wait(48, self.ps.at[slot])
        self.wait(48, self.pr.at[slot])
        x = self.at_x(2)
        for d, dx in enumerate(HOPS):
            to = self.h1u.at[two, d], self.h1d.at[two, d]
            self.ship(b, x, d, 2, self.both(b, x, d, 2), to, self.h1s.at[two], self.h1r.at[two, d], self.p.at(dx=dx))
        for d, dx in enumerate(HOPS):
            self.hop(b, d, 1 - d, self.both(b, self.at_x(dx), 1 - d, 2))

    def second(self, b):
        two = odd(b)
        for d in PAIR:
            self.wait(6, self.h1r.at[two, d])
        for d, dx in enumerate(HOPS):
            up, down = self.both(b, self.at_x(dx), d, 2)
            self.hop(b, d, d, (up + self.h1u[two, d].astype(F32), down + self.h1d[two, d].astype(F32)))

    def chip_sum(self, b, q):
        slot = slot3(b)
        cols, rows = self.cut(q, QUARTERS)
        up, down = self.both(b, self.p.x, q, QUARTERS)
        for d in PAIR:
            up, down = up + self.h2u[slot, d, :, :, cols].astype(F32), down + self.h2d[slot, d, rows, :].astype(F32)
        return up, down

    def third(self, b):
        slot, two = slot3(b), odd(b)
        self.wait(12, self.h1s.at[two])
        self.wait(24, self.h2s.at[slot])
        for d in PAIR:
            self.wait(12, self.h2r.at[slot, d])
        for n in range(self.p.nr - 1):
            q = (self.p.r + n + 1) % self.p.nr
            to = self.su.at[two, n], self.sd.at[two, n]
            self.ship(b, self.p.x, q, QUARTERS, self.chip_sum(b, q), to, self.ss.at[two], self.sr.at[two, n], self.p.at(dy=n + 1))

    def fourth(self, b):
        two = odd(b)
        layer, n = self.layers - 1 - b // self.nb, b % self.nb
        j = 4 * (odd(n)) + n // 2
        self.wait(9, self.ss.at[two])
        for n in range(self.p.nr - 1):
            self.wait(3, self.sr.at[two, n])

        @pl.when(b >= 2)
        def _():
            self.final_sent(two)

        q = self.p.r
        up, down = self.chip_sum(b, q)
        for n in range(self.p.nr - 1):
            up, down = up + self.su[two, n].astype(F32), down + self.sd[two, n].astype(F32)
        self.fu[two] = up.astype(BF16)
        self.fd[two] = down.astype(BF16)

        up_to = self.out_up.at[:, layer, :, lanes_of(LANES * (self.nb * q + j), LANES)]
        share = self.out_down.shape[1]
        first = self.rows * (2 * j + self.p.c)
        owner = first // share
        quarter = self.rows // QUARTERS
        down_to = self.out_down.at[layer, rows_of(first + quarter * q - share * owner, quarter), :]
        for dy in range(1, self.p.nr):
            send(self.fu.at[two], up_to, self.fs.at[two], self.ru.at[0], self.p.at(dy=dy))
            peer = {"r": (self.p.r + dy) % self.p.nr, "s": 2 * self.p.x + owner}
            send(self.fd.at[two], down_to, self.fs.at[two], self.rd.at[0], peer)
        pltpu.make_async_copy(self.fu.at[two], up_to, self.fl.at[two]).start()

        @pl.when(owner == self.p.c)
        def _():
            pltpu.make_async_copy(self.fd.at[two], down_to, self.fx.at[two]).start()

        @pl.when(owner != self.p.c)
        def _():
            send(self.fd.at[two], down_to, self.fx.at[two], self.rd.at[0], self.p.at(dc=1))

    def final_sent(self, two):
        for n, sem in ((9, self.fs), (2, self.fl), (1, self.fx)):
            self.wait(n, sem.at[two])


def backward_kernel(
    nr, ns, dy_h, dyt_h, a0t_h, xt_h, a1_h, a1t_h, h1t_h, f_h, act_h, wup_in, wd_in, dx_h, gup_h, gd_h, wup_h, wd_h, kept_h,
    a, at, dy, dyt, ht, dat, f, act, dg, du, wup, wd, tu, td, pu, pd, h1u, h1d, h2u, h2d, su, sd, fu, fd,
    ps, pr, h1s, h1r, h2s, h2r, ss, sr, fs, fl, fx, ru, rd, x1s, x1r, x2s, x2r, ys, yr, ds, dr, _, io, wsem, ksem, fsem,
):
    place = Place(nr, ns)
    tokens, d = a.shape
    layers, nb = wup_h.shape[:2]
    steps = layers * nb
    halves = [(h.at[pl.ds(n, BIG), :], v.at[pl.ds(n, BIG), :]) for n in range(0, tokens, BIG) for h, v in ((a1_h, a), (dy_h, dy))]
    loads = copies(halves + [(a1t_h, at), (dyt_h, dyt), (h1t_h, ht)], io)
    gather = Gather(place, (wup_h, wd_h), gup_h.shape[2], gd_h.shape[1], (x1s, x1r, x2s, x2r, ys, yr, ds, dr, None))
    ahead = nb + AHEAD

    def block_of(b):
        return gather.piece(steps - nb + b % nb - (b // nb) * nb)

    def load_up(b):
        layer, j, _ = block_of(b)
        return pltpu.make_async_copy(wup_h.at[layer, j], wup.at[odd(b)], wsem.at[odd(b), 0])

    def load_down(b):
        layer, j, _ = block_of(b)
        return copies([(wd_h.at[layer, rows_of((q * nb + j) * LANES, LANES), :], wd.at[odd(b), pl.ds(q * LANES, LANES), :]) for q in range(QUARTERS)], wsem.at[2 + odd(b)])

    start((*loads[:2], load_up(0), *load_down(0), *loads[2:4]))
    greet([place.at(dc=1)] + [place.at(dx=hop) for hop in HOPS] + [place.at(dy=hop, dc=c) for hop in range(1, nr) for c in CORES])
    reduce = Reduce(
        place, wup_h.at[0, :, 0], nb, layers, (tu, td, pu, pd, h1u, h1d, h2u, h2d, su, sd, fu, fd), (gup_h, gd_h),
        (ps, pr, h1s, h1r, h2s, h2r, ss, sr, fs, fl, fx, ru, rd),
    )
    dat[...] = jnp.zeros_like(dat)
    wait(loads[:2])

    def layer_end(begin, end, last):
        def chunk(n, carry):
            cols = lanes_of(n * SMALL, SMALL)

            def part(rows):
                return ht[rows, cols].astype(F32), dat[rows, cols].astype(BF16).astype(F32)

            def sums(i, so_far):
                h, da = part(rows_of(i * LANES, LANES))
                return tuple(s + jnp.sum((v * h).reshape(-1, 8, SMALL), 0) for s, v in zip(so_far, (h, da)))

            none = jnp.zeros((8, SMALL), F32)
            square, cross = (jnp.sum(v, 0, keepdims=True) for v in lax.fori_loop(0, d // LANES, sums, (none, none)))
            scale = lax.rsqrt(square / d + 1e-6)
            h, da = part(ALL)
            v = dyt[:, cols].astype(F32) + scale * (da - h * scale * (scale * cross / d))
            v = v.astype(BF16)
            if not last:
                dyt[:, cols] = v
                dat[:, cols] = jnp.zeros((d, SMALL), F32)
            dy[cols, :] = v.T
            return carry

        with jax.named_scope("end"):
            lax.fori_loop(begin // SMALL, end // SMALL, chunk, 0)

    def keep(k):
        return copies([(v, kept_h.at[n, k - nb]) for n, v in enumerate((dg, du))], ksem)

    def load_f(q):
        rows = rows_of(q % QUARTERS * BLOCK, BLOCK)
        return copies([(f_h.at[e, q // QUARTERS, rows, :], f.at[slot3(q), e]) for e in PAIR], fsem.at[slot3(q)])

    def load_act(k):
        return pltpu.make_async_copy(act_h.at[k - nb], act, ksem.at[2])

    def compute(k, between):
        slot = odd(k)
        wait((load_up(k), *load_down(k)))

        def chunk(n, carry):
            for part in PARTS:
                rows = rows_of(n * BIG + part.start, BLOCK)
                for cols in COLUMNS:
                    g = dot(a[rows, :], wup[slot, 0, :, cols])
                    u = dot(a[rows, :], wup[slot, 1, :, cols])
                    e = dot_t(dy[rows, :], wd[slot, cols, :]).astype(BF16).astype(F32)
                    sig, s = gate(g)
                    act[rows, cols] = (s * u).astype(BF16)
                    dg[rows, cols] = (e * u * (sig + s - s * sig)).astype(BF16)
                    du[rows, cols] = (e * s).astype(BF16)

            @pl.when(n == 0)
            def _():
                between()

            return carry

        lax.fori_loop(0, tokens // BIG, chunk, 0)

    def compute_last(k):
        slot = odd(k)
        wait((load_up(k), *load_down(k)))

        @pl.when(k > nb)
        def _():
            wait(keep(k - 1))

        def chunk(n, carry):
            q = (k - nb) * QUARTERS + n
            wait(load_f(q))

            @pl.when(q + 2 < nb * QUARTERS)
            def _():
                start(load_f(q + 2))

            for cols in COLUMNS:
                e = dot_t(dy[rows_of(n * BLOCK, BLOCK), :], wd[slot, cols, :]).astype(BF16).astype(F32)
                for n_, v in enumerate((du, dg)):
                    v[rows_of(n * BLOCK, BLOCK), cols] = (e * f[slot3(q), n_, :, cols]).astype(BF16)
            return carry

        lax.fori_loop(0, tokens // BLOCK, chunk, 0)
        @pl.when(k < steps - 1)
        def _():
            start(keep(k))

    def terms(k, before):
        slot = slot3(k)

        @pl.when(k >= nb)
        def _():
            load_act(k).wait()

        for cols in COLUMNS:
            td[slot, cols, :] = dot(dyt[...], act[:, cols]).astype(BF16).T
        for n, left in enumerate((dg, du)):
            for cols in COLUMNS:
                tu[slot, n, :, cols] = dot(at[...], left[:, cols]).astype(BF16)
        reduce.pair_up(k)
        before()
        reduce.pair_down(k)

    def back(k):
        slot = odd(k)
        for n in range(tokens // BLOCK):
            cols = pl.ds(n * BLOCK, BLOCK)
            dat[:, cols] += dot_t(wup[slot, 0], dg[cols, :]) + dot_t(wup[slot, 1], du[cols, :])

    def back_half(half, slot, first):
        rows, cols = rows_of(first, BIG), lanes_of(half * BIG, BIG)
        dat[:, cols] += dot_t(wup[slot, 0], dg[rows, :]) + dot_t(wup[slot, 1], du[rows, :])

    def later(t):
        half = jnp.where(t == 2, 0, 1)
        j = jnp.where(t == 2, nb - 2, t - 3)
        _, order, _ = gather.piece(j)
        slot = odd(t)
        yield pltpu.make_async_copy(wup_h.at[0, order], wup.at[slot], wsem.at[slot, 0])
        for n, v in enumerate((dg, du), 1):
            yield pltpu.make_async_copy(kept_h.at[n - 1, j, rows_of(half * BIG, BIG), :], v.at[rows_of(slot * BIG, BIG), :], wsem.at[slot, n])

    def back_later(t):
        @pl.when(t >= 2)
        def _():
            wait(later(t))

        @pl.when((t >= 1) & (t < nb + 1))
        def _():
            start(later(t + 1))

        slot = odd(t)
        back_half(jnp.where((t == 0) | (t == 2), 0, 1), jnp.where(t == 0, 1, slot), slot * BIG)

    def done(half):
        rows = pl.ds(half * BIG, BIG)
        return pltpu.make_async_copy(dy.at[rows, :], dx_h.at[rows, :], io.at[half])

    def step(k, carry):
        t = k - steps

        def stage(run, lag, *late):
            b = k - lag
            now = (k >= lag) & (k < steps)
            for n, when in enumerate(late):
                now = now | (t == when)
                b = jnp.where(t == when, steps - len(late) + n, b)

            @pl.when(now)
            def _():
                with jax.named_scope("r_" + run.__name__):
                    run(b)

        def tick(*entries):
            for pieces, when, run in entries:

                @pl.when(k == when)
                def _():
                    with jax.named_scope("gather"):
                        for i in pieces:
                            run(ahead + i)

        one, two, rest = (0,), (1,), range(2, steps - ahead)

        def arrived(i):
            wait_for(gather.units(36), dr.at[i])

        tick((one, 0, gather.first), (two, 0, gather.first), (one, 1, gather.fourth), (two, 1, gather.third), (rest, 3, gather.fourth))

        def between():
            @pl.when(k == 0)
            def _():
                wait(loads[2:4])
                start(loads[4:])

            stage(reduce.third, 2)

        @pl.when(k < nb)
        def _():
            with jax.named_scope("compute"):
                compute(k, between)

        @pl.when((k >= nb) & (k < steps))
        def _():
            with jax.named_scope("compute_last"):
                compute_last(k)

        tick((one, 0, gather.second), (two, 1, gather.fourth), (rest, 2, gather.third))

        @pl.when((k >= nb - 1) & (k + 1 < steps))
        def _():
            start((load_up(k + 1), *load_down(k + 1)))

        stage(reduce.first, 1, 1)

        @pl.when(k >= nb)
        def _():
            stage(reduce.third, 2, 2, 6)


        @pl.when(k == 0)
        def _():
            wait(loads[4:])

        @pl.when(k < steps)
        def _():
            with jax.named_scope("terms"):
                terms(k, lambda: stage(reduce.fourth, 2))

        @pl.when(k >= steps)
        def _():
            stage(reduce.fourth, steps, 5, nb + 2)

        stage(reduce.second, 1, 3)
        tick((one, 0, gather.third), (two, 0, gather.second), (rest, 0, gather.first), ((0, 1), 1, arrived), (rest, 1, gather.second), (rest, 3, arrived))

        @pl.when((k >= nb - 1) & (k + 1 < steps))
        def _():
            load_act(k + 1).start()

        @pl.when(k < nb - 1)
        def _():
            start((load_up(k + 1), *load_down(k + 1)))

        @pl.when(k < nb)
        def _():
            with jax.named_scope("back"):
                back(k)

        @pl.when((k >= nb) & (k < steps - 2))
        def _():
            with jax.named_scope("back_half"):
                back_half(0, odd(k), 0)

        @pl.when(k == nb - 1)
        def _():
            load = pltpu.make_async_copy(a0t_h, at, io.at[0])
            start((load, *load_f(0), *load_f(1)))
            layer_end(0, tokens, False)
            turned.start()
            load.wait()

        @pl.when((t >= 0) & (t < nb + 2))
        def _():
            with jax.named_scope("back_later"):
                back_later(t)

        return carry

    turned = pltpu.make_async_copy(xt_h, ht, io.at[4])
    lax.fori_loop(0, steps + nb + 3, step, 0)
    turned.wait()
    for half in PAIR:
        layer_end(half * BIG, half * BIG + BIG, True)
        done(half).start()

    def drain(i, carry):
        gather.sent(i, 12)
        return carry

    lax.fori_loop(ahead, steps, drain, 0)
    for two in PAIR:
        reduce.final_sent(two)
    reduce.wait(6 * steps, ru.at[0])
    reduce.wait(48, rd.at[0])
    wait((done(0), done(1)))


def backward(mesh, dy, dyt, a0t, xt, a1, a1t, h1t, f, act, wup, wd):
    nr, ns = mesh.shape["r"], mesh.shape["s"]
    nx = ns // 2
    tokens, d = dy.shape
    layers, nb = wup.shape[:2]
    hidden = nb * BLOCK
    m, share, rows = d // ns, hidden // ns, BLOCK // ns
    outs = (array(tokens, d), array(2, layers, m, hidden), array(layers, share, d), array(*wup.shape), array(*wd.shape), array(2, nb, tokens, BLOCK))
    scratch = [
        *[vmem(tokens, d), vmem(d, tokens)] * 2, vmem(d, tokens), vmem(d, tokens, dtype=F32), vmem(3, 2, BLOCK, BLOCK, dtype=F32), *[vmem(tokens, BLOCK)] * 3,
        vmem(2, 2, d, BLOCK), vmem(2, BLOCK, d), vmem(3, 2, d, BLOCK), vmem(3, BLOCK, d), vmem(3, nx, 2, m, BLOCK), vmem(3, nx, rows, d),
        vmem(2, 2, 2, m, BLOCK // 2), vmem(2, 2, rows // 2, d), vmem(3, 2, 2, m, BLOCK), vmem(3, 2, rows, d),
        vmem(2, nr - 1, 2, m, LANES), vmem(2, nr - 1, rows // QUARTERS, d), vmem(2, 2, m, LANES), vmem(2, rows // QUARTERS, d),
        *sems(3, 3, 2, (2, 2), 3, (3, 2), 2, (2, nr - 1), 2, 2, 2, 1, 1), *gather_sems(layers * nb), *sems(8, (QUARTERS, QUARTERS), 3, (3, 2)),
    ]
    return call(backward_kernel, mesh, "backward", 1, outs, scratch, (dy, dyt, a0t, xt, a1, a1t, h1t, f, act, wup, wd), {9: 3, 10: 4})[:3]


def deliver_kernel(nr, ns, dx_h, gup_h, gd_h, out_x, out_gate, out_up, out_down, x, up, down, arrive, leave):
    jobs = []
    for h, out, v in ((dx_h, out_x, x), (gup_h.at[0], out_gate, up.at[0]), (gup_h.at[1], out_up, up.at[1]), (gd_h, out_down, down)):
        size = BIG if out is out_x else 1
        for n in range(0, out.shape[0], size):
            part = pl.ds(n, size)
            jobs.append((h.at[part], v.at[part], out.at[part]))
    loads = copies([job[:2] for job in jobs], arrive)
    stores = copies([job[1:] for job in jobs], leave)
    start(loads)
    for load, store in zip(loads, stores):
        load.wait()
        store.start()
    wait(stores)


def deliver(mesh, dx, gup, gd):
    up = gup.shape[1:]
    scratch = [vmem(*v.shape) for v in (dx, gup, gd)] + sems(8, 8)
    return call(deliver_kernel, mesh, "deliver", None, (array(*dx.shape), array(*up), array(*up), array(*gd.shape)), scratch, (dx, gup, gd))


def solution(mesh):
    def step(x, dy, *weights):
        xt, dyt, a0t, a1, a1t, h1t, wup, wd, f, act = forward(mesh, x[0], dy[0], *weights)
        results = backward(mesh, dy[0], dyt, a0t, xt, a1, a1t, h1t, f, act, wup, wd)
        dx, *by_weights = deliver(mesh, *results)
        return dx[None], *by_weights

    states, cut = P(("rep", "r", "s"), None, None), P(None, "s", None)
    return jax.shard_map(
        step,
        mesh=mesh,
        in_specs=(states, states) + (cut,) * 3,
        out_specs=(states,) + (P("rep", "s", None),) * 3,
        check_vma=False,
    )
```
